512 devices in a mesh: groups: 2 (over y), gx: 64 (over z, core), gy: 4 (over x).
Axes of the slice: x: 4, y: 2, z: 32, core: 2. Of those that a mesh axis runs over, the one named last changes fastest.
The devices are a block of a 4x8x32 slice.
Arguments:
- thermal_deviation: float32 [32, 256, 8192], P('groups', 'gy', 'gx'), parts along dimension 0, may hold values from -6 to 6
- brine_content: float32 [32, 256, 8192], P('groups', 'gy', 'gx'), parts along dimension 0, may hold values from 0.2 to 2.4
- current_components: float32 [4, 16, 256, 8192], P('groups', None, 'gy', 'gx'), parts along dimension 0, may hold values from -4 to 4
- sea_indicator: int32 [256, 8192], P('gy', 'gx'), may hold values from 0 to 1, as said below
- flooded_layer_number: int32 [256, 8192], P('gy', 'gx'), may hold values from 1 to 16
- footprint_square_metres: float32 [256, 8192], P('gy', 'gx'), may hold values from 0.5 to 5
- rainfall_input: float32 [256, 8192], P('gy', 'gx'), may hold values from -2 to 3.5
- seam_partner_index: int32 [8192], P('gx'), may hold values from 0 to 8191, as said below
Outputs:
- temperature_next: float32 [32, 256, 8192], P('groups', 'gy', 'gx'), parts along dimension 0
- salinity_next: float32 [32, 256, 8192], P('groups', 'gy', 'gx'), parts along dimension 0
The draws below stay inside these ranges and needn't reach their ends.
There are 2 independent parts, one for each index of `groups`. The reference program is written for one: setup_inputs(seed, part) draws one part's arguments, and reference() takes and returns one part's arrays. A program takes and returns all parts, laid end to end along the dimension named above; an argument that names none is the same for every part. Nothing has to cross between parts.
Inputs may be any that keep to these rules, and one draw needn't show every extreme that they name: `sea_indicator`: at least one column is ocean. seam_partner_index[x] = (s - x) mod 8192 for one s of each draw with s mod 128 = 127; the map is its own inverse and has no fixed point.
All inputs are finite; a program needn't handle non-finite values.
Results may differ from the reference program's by a relative error of at most 0.00002.
Values sent between devices are 32-bit elements; how exact they have to be, the bound alone decides.
No kernel may reach another device: no remote copies, remote signals or barrier semaphores. Data moves between devices by JAX's collectives and lax.ppermute only.
A program may use at most 64 MiB of HBM per device.

```python
import math
import jax
import jax.numpy as jnp

SEA_LAYER_TOTAL = 16
CX = 128
PARALLEL_TOTAL = 256
MERIDIAN_TOTAL = 8192


def draw_brine_content(key, part):
    longitude = jnp.arange(MERIDIAN_TOTAL, dtype=jnp.float32) / MERIDIAN_TOTAL
    zonal_trend = 0.5 + longitude
    factor = jax.random.uniform(key, (SEA_LAYER_TOTAL, PARALLEL_TOTAL, MERIDIAN_TOTAL), jnp.float32, 0.6, 1.4)
    return (zonal_trend * factor).astype(jnp.float32)


def draw_rainfall_input(key, part):
    second = jax.random.fold_in(jax.random.fold_in(key, 11), 1)
    longitude = jnp.arange(MERIDIAN_TOTAL, dtype=jnp.float32) / MERIDIAN_TOTAL
    zonal_trend = 0.5 + longitude
    rough_noise = jnp.clip(0.5 * jax.random.normal(second, (PARALLEL_TOTAL, MERIDIAN_TOTAL), jnp.float32), -2.0, 2.0)
    return (zonal_trend + rough_noise).astype(jnp.float32)


def draw_sea_indicator(key, part):
    first, second = jax.random.split(jax.random.fold_in(key, 23))
    ocean_draw = (jax.random.randint(first, (PARALLEL_TOTAL, MERIDIAN_TOTAL), 0, 4) < 3).astype(jnp.int32)
    chosen = jax.random.randint(second, (), 0, PARALLEL_TOTAL * MERIDIAN_TOTAL)
    flat_index = jnp.arange(PARALLEL_TOTAL * MERIDIAN_TOTAL, dtype=jnp.int32).reshape(PARALLEL_TOTAL, MERIDIAN_TOTAL)
    return jnp.where(flat_index == chosen, 1, ocean_draw).astype(jnp.int32)


def draw_seam_partner_index(key, part):
    block_choice = jax.random.randint(jax.random.fold_in(key, 37), (), 0, MERIDIAN_TOTAL // CX)
    centre = CX * block_choice + CX - 1
    return ((centre - jnp.arange(MERIDIAN_TOTAL, dtype=jnp.int32)) % MERIDIAN_TOTAL).astype(jnp.int32)


def place_ends(drawn, stream_key, low, top_value):
    place = [jax.random.randint(jax.random.fold_in(stream_key, axis), (), 0, length) for axis, length in enumerate(drawn.shape)]
    widest = drawn.shape.index(max(drawn.shape))
    beside = place[:widest] + [(place[widest] + 1) % drawn.shape[widest]] + place[widest + 1:]
    return drawn.at[tuple(place)].set(low).at[tuple(beside)].set(top_value)


def shard_levels(stream_key, shape, cuts, least, largest):
    level, own = 1.0, jax.random.fold_in(stream_key, 6)
    for position, blocks in cuts:
        draws = jnp.exp(jax.random.uniform(jax.random.fold_in(own, position), (blocks,), jnp.float32, least / len(cuts), largest / len(cuts)))
        level = level * jnp.repeat(draws, shape[position] // blocks).reshape([-1 if axis == position else 1 for axis in range(len(shape))])
    return level


def noise(rng, dims, scale, bound, pieces=(), kind=jnp.bfloat16):
    entries = scale * jax.random.normal(rng, dims, jnp.float32)
    if pieces:
        entries = entries * shard_levels(rng, dims, pieces, -0.22, 0.18)
    return jnp.clip(entries, -bound, bound).astype(kind)


def setup_inputs(seed: int = 0, part: int = 0) -> dict:
    splits = jax.random.split(jax.random.key(seed), 9)
    part_keys = jax.random.split(jax.random.fold_in(splits[8], part), 9)
    thermal_deviation = noise(part_keys[0], (SEA_LAYER_TOTAL, PARALLEL_TOTAL, MERIDIAN_TOTAL), 1.0, 6.0, ((1, 4), (2, 64)), jnp.float32)
    brine_content = draw_brine_content(jax.random.fold_in(jax.random.fold_in(splits[8], part), 71), part)
    current_components = noise(part_keys[2], (2, SEA_LAYER_TOTAL, PARALLEL_TOTAL, MERIDIAN_TOTAL), 1.0, 4.0, ((2, 4), (3, 64)), jnp.float32)
    sea_indicator = draw_sea_indicator(jax.random.fold_in(splits[8], 71), part)
    flooded_layer_number = place_ends(jax.random.randint(splits[4], (PARALLEL_TOTAL, MERIDIAN_TOTAL), 1, SEA_LAYER_TOTAL + 1), jax.random.fold_in(splits[4], 1), 1, SEA_LAYER_TOTAL).astype(jnp.int32)
    footprint_square_metres = jnp.clip(jnp.exp(math.log(5.0) - 2.3025851 * jax.random.uniform(splits[5], (PARALLEL_TOTAL, MERIDIAN_TOTAL), jnp.float32) ** shard_levels(splits[5], (PARALLEL_TOTAL, MERIDIAN_TOTAL), ((0, 4), (1, 64)), -0.2, 0.2)), 0.5, 5.0)
    rainfall_input = draw_rainfall_input(jax.random.fold_in(splits[8], 71), part)
    seam_partner_index = draw_seam_partner_index(jax.random.fold_in(splits[8], 71), part)
    return {"thermal_deviation": thermal_deviation, "brine_content": brine_content, "current_components": current_components, "sea_indicator": sea_indicator, "flooded_layer_number": flooded_layer_number, "footprint_square_metres": footprint_square_metres, "rainfall_input": rainfall_input, "seam_partner_index": seam_partner_index}


time_step = 0.25
diffusivity = 0.5
vertical_mixing = 0.3
top_thickness = 0.5


def face_flux(near_cells, far_cells, face_speed, near_wet, far_wet):
    upwind = jnp.maximum(face_speed, 0.0) * near_cells + jnp.minimum(face_speed, 0.0) * far_cells
    return near_wet * far_wet * (upwind - diffusivity * (far_cells - near_cells))


def reference(thermal_deviation, brine_content, current_components, sea_indicator, flooded_layer_number, footprint_square_metres, rainfall_input, seam_partner_index):
    layer_stack_number = thermal_deviation.shape[0]
    stacked_layer_number = (sea_indicator * flooded_layer_number).astype(jnp.float32)
    level_index = jnp.arange(layer_stack_number, dtype=jnp.float32)
    wet_cells = (level_index[:, None, None] < stacked_layer_number[None]).astype(jnp.float32)
    carried_quantity = jnp.stack([thermal_deviation, brine_content])
    east_tracer = jnp.roll(carried_quantity, -1, axis=3)
    east_wet = jnp.roll(wet_cells, -1, axis=2)
    east_flux = face_flux(carried_quantity, east_tracer, current_components[0], wet_cells, east_wet)
    west_flux = jnp.roll(east_flux, 1, axis=3)
    fold_tracer = carried_quantity[:, :, -1, :][:, :, seam_partner_index]
    fold_wet = wet_cells[:, -1, :][:, seam_partner_index]
    fold_velocity = current_components[1][:, -1, :][:, seam_partner_index]
    north_tracer = jnp.concatenate([carried_quantity[:, :, 1:], fold_tracer[:, :, None]], axis=2)
    north_wet = jnp.concatenate([wet_cells[:, 1:], fold_wet[:, None]], axis=1)
    fold_speed = 0.5 * (current_components[1][:, -1, :] - fold_velocity)
    north_speed = jnp.concatenate([current_components[1][:, :-1], fold_speed[:, None]], axis=1)
    north_flux = face_flux(carried_quantity, north_tracer, north_speed, wet_cells, north_wet)
    south_flux = jnp.concatenate([jnp.zeros_like(north_flux[:, :, :1]), north_flux[:, :, :-1]], axis=2)
    vertical = wet_cells[:-1] * wet_cells[1:] * vertical_mixing * (carried_quantity[:, :-1] - carried_quantity[:, 1:])
    zero_layer = jnp.zeros_like(vertical[:, :1])
    from_above = jnp.concatenate([zero_layer, vertical], axis=1)
    to_below = jnp.concatenate([vertical, zero_layer], axis=1)
    tendency = time_step / footprint_square_metres * (west_flux - east_flux + south_flux - north_flux) + time_step * (from_above - to_below)
    updated = carried_quantity + wet_cells * tendency
    wet_area = footprint_square_metres * sea_indicator.astype(jnp.float32)
    total_area = jnp.sum(wet_area)
    mean_fresh = jnp.sum(wet_area * rainfall_input) / total_area
    balanced = rainfall_input - mean_fresh
    surface = brine_content[0]
    total_salt = jnp.sum(wet_area * surface * balanced)
    virtual = -surface * balanced + total_salt / total_area
    surface_next = updated[1, 0] + time_step / top_thickness * virtual * wet_cells[0]
    salinity_next = jnp.concatenate([surface_next[None], updated[1, 1:]], axis=0)
    return (updated[0], salinity_next)
```

```python
import functools

import jax
import jax.numpy as jnp
from jax import lax
from jax.experimental import pallas as pl
from jax.experimental.pallas import tpu as pltpu
from jax.sharding import PartitionSpec as P

time_step = 0.25
diffusivity = 0.5
vertical_mixing = 0.3
top_thickness = 0.5

VMEM = pl.BlockSpec(memory_space=pltpu.VMEM)
LANES = 128


def lane_of(shape):
    return lax.broadcasted_iota(jnp.int32, shape, len(shape) - 1)


def sums_kernel(surface, sea, area, rain, out):
    wet_area = area[...] * sea[...].astype(jnp.float32)
    salt = wet_area * surface[0]
    rain_now = rain[...]
    lane = lane_of((1, LANES))
    packed = jnp.zeros((1, LANES), jnp.float32)
    for place, field in enumerate((wet_area, wet_area * rain_now, salt * rain_now, salt)):
        total = jnp.sum(jnp.sum(field, axis=0, keepdims=True), axis=1, keepdims=True)
        packed = jnp.where(lane == place, total, packed)
    out[...] = packed


def local_sums(brine, sea, area, rain):
    rows, width = sea.shape
    plane = pl.BlockSpec((rows, width), lambda i: (0, 0))
    return pl.pallas_call(
        sums_kernel,
        grid=(1,),
        in_specs=[pl.BlockSpec((1, rows, width), lambda i: (0, 0, 0)), plane, plane, plane],
        out_specs=pl.BlockSpec((1, LANES), lambda i: (0, 0)),
        out_shape=jax.ShapeDtypeStruct((1, LANES), jnp.float32),
        name="local_sums",
    )(brine, sea, area, rain)


def mirrored(rows):
    lane = lane_of(rows.shape)
    bit = 1
    while bit < LANES:
        low = (lane // bit) % 2 == 0
        rows = jnp.where(low, pltpu.roll(rows, LANES - bit, 1), pltpu.roll(rows, bit, 1))
        bit *= 2
    return rows


def column_pack(planes, lane_number):
    lane = lane_of((8, LANES))
    blocks = planes[0].shape[0] // 8
    packed = jnp.zeros((8, LANES), jnp.float32)
    for level, plane in enumerate(planes):
        for block in range(blocks):
            place = level * blocks + block
            tile = plane[8 * block : 8 * block + 8]
            moved = pltpu.roll(tile, (place - lane_number) % LANES, 1)
            packed = jnp.where(lane == place, moved, packed)
    return packed


def pack_kernel(heat, salt, currents, sea, layers, west, east, south, north, fold):
    levels, rows, _ = heat.shape
    depth = (sea[...] * layers[...]).astype(jnp.float32)
    heat_planes = [heat[k] for k in range(levels)]
    salt_planes = [salt[k] for k in range(levels)]
    speed_planes = [currents[0, k] for k in range(levels)]
    depth_planes = [depth] * levels
    west[0:8] = column_pack(heat_planes, 0)
    west[8:16] = column_pack(salt_planes, 0)
    west[16:24] = column_pack(depth_planes, 0)
    east[0:8] = column_pack(heat_planes, LANES - 1)
    east[8:16] = column_pack(salt_planes, LANES - 1)
    east[16:24] = column_pack(depth_planes, LANES - 1)
    east[24:32] = column_pack(speed_planes, LANES - 1)
    last = rows - 1
    for k in range(levels):
        south[k : k + 1] = heat[k, 0:1]
        south[levels + k : levels + k + 1] = salt[k, 0:1]
        north[k : k + 1] = heat[k, last:rows]
        north[levels + k : levels + k + 1] = salt[k, last:rows]
        north[2 * levels + 8 + k : 2 * levels + 9 + k] = currents[1, k, last:rows]
    south[2 * levels : 2 * levels + 8] = jnp.broadcast_to(depth[0:1], (8, LANES))
    north[2 * levels : 2 * levels + 8] = jnp.broadcast_to(depth[last:rows], (8, LANES))
    fold[...] = mirrored(north[...])


def packs(heat, salt, currents, sea, layers):
    levels, rows, width = heat.shape
    shapes = (24, 32, 2 * levels + 8, 3 * levels + 8, 3 * levels + 8)
    return pl.pallas_call(
        pack_kernel,
        in_specs=[VMEM] * 5,
        out_specs=[VMEM] * 5,
        out_shape=[jax.ShapeDtypeStruct((n, LANES), jnp.float32) for n in shapes],
        name="edge_packs",
    )(heat, salt, currents, sea, layers)


def open_flux(near, far, forward, backward):
    return forward * near + backward * far - diffusivity * (far - near)


def edge_flux(near, far, speed, near_depth, far_depth, level):
    wet = (level < jnp.minimum(near_depth, far_depth)).astype(jnp.float32)
    return wet * open_flux(near, far, jnp.maximum(speed, 0.0), jnp.minimum(speed, 0.0))


def step_kernel(
    flags, heat, salt, currents, sea, layers, area,
    west_own, east_own, west_halo, east_halo, south_halo, north_halo, fold_halo,
    heat_out, salt_out,
):
    levels, rows, _ = heat.shape
    blocks = rows // 8
    lane = lane_of((rows, LANES))
    row = lax.broadcasted_iota(jnp.int32, (rows, LANES), 0)
    first_lane, last_lane = lane == 0, lane == LANES - 1
    first_row, last_row = row == 0, row == rows - 1
    is_top = flags[0] == 1
    depth = (sea[...] * layers[...]).astype(jnp.float32)
    base = 2 * levels
    north_depth = jnp.where(is_top, fold_halo[base : base + 1], north_halo[base : base + 1])
    south_depth = south_halo[base : base + 1]
    depth_north = jnp.where(last_row, north_depth, pltpu.roll(depth, rows - 1, 0))
    open_north = jnp.minimum(depth, depth_north)
    open_south = jnp.minimum(depth[0:1], south_depth)
    open_east = jnp.where(last_lane, 0.0, jnp.minimum(depth, pltpu.roll(depth, LANES - 1, 1)))
    per_area = time_step / area[...]
    edge_level = (lane_of((8, LANES)) // blocks).astype(jnp.float32)
    west_edge, east_edge = [], []
    for f in range(2):
        own_west, own_east = west_own[8 * f : 8 * f + 8], east_own[8 * f : 8 * f + 8]
        west_edge.append(
            edge_flux(west_halo[8 * f : 8 * f + 8], own_west, west_halo[24:32], west_halo[16:24], west_own[16:24], edge_level)
        )
        east_edge.append(
            edge_flux(own_east, east_halo[8 * f : 8 * f + 8], east_own[24:32], east_own[16:24], east_halo[16:24], edge_level)
        )
    fields = (heat, salt)
    above = [None, None]
    for k in range(levels):
        level = float(k)
        east_speed = currents[0, k]
        north_speed = currents[1, k]
        fold_speed = 0.5 * (north_speed[rows - 1 : rows] - fold_halo[base + 8 + k : base + 9 + k])
        top_speed = jnp.where(is_top, fold_speed, north_speed[rows - 1 : rows])
        north_speed = jnp.where(last_row, top_speed, north_speed)
        south_speed = south_halo[base + 8 + k : base + 9 + k]
        east_up, east_down = jnp.maximum(east_speed, 0.0), jnp.minimum(east_speed, 0.0)
        north_up, north_down = jnp.maximum(north_speed, 0.0), jnp.minimum(north_speed, 0.0)
        east_wet = level < open_east
        north_wet = level < open_north
        for f in range(2):
            cells = fields[f][k]
            at = f * levels + k
            east_flux = jnp.where(
                east_wet, open_flux(cells, pltpu.roll(cells, LANES - 1, 1), east_up, east_down), 0.0
            )
            west_flux = pltpu.roll(east_flux, 1, 1)
            west_columns, east_columns = [], []
            for block in range(blocks):
                place = k * blocks + block
                west_columns.append(pltpu.roll(west_edge[f], (-place) % LANES, 1))
                east_columns.append(pltpu.roll(east_edge[f], (LANES - 1 - place) % LANES, 1))
            west_flux = jnp.where(first_lane, jnp.concatenate(west_columns, axis=0), west_flux)
            east_flux = jnp.where(last_lane, jnp.concatenate(east_columns, axis=0), east_flux)
            top_cells = jnp.where(is_top, fold_halo[at : at + 1], north_halo[at : at + 1])
            northern = jnp.where(last_row, top_cells, pltpu.roll(cells, rows - 1, 0))
            north_flux = jnp.where(north_wet, open_flux(cells, northern, north_up, north_down), 0.0)
            first_flux = edge_flux(south_halo[at : at + 1], cells[0:1], south_speed, open_south, open_south, level)
            south_flux = jnp.where(first_row, first_flux, pltpu.roll(north_flux, 1, 0))
            change = per_area * (west_flux - east_flux + south_flux - north_flux)
            if k > 0:
                change = change + time_step * above[f]
            if k < levels - 1:
                below = jnp.where(level + 1.0 < depth, vertical_mixing * (cells - fields[f][k + 1]), 0.0)
                change = change - time_step * below
                above[f] = below
            result = cells + jnp.where(level < depth, change, 0.0)
            (heat_out, salt_out)[f][k] = result


def final_kernel(salt_next, surface, rain, sea, totals, out):
    lane = lane_of((1, LANES))

    def total(place):
        return jnp.sum(jnp.where(lane == place, totals[...], 0.0), axis=1, keepdims=True)

    total_area, total_fresh, salt_fresh, salt_only = (total(place) for place in range(4))
    mean_fresh = total_fresh / total_area
    total_salt = salt_fresh - mean_fresh * salt_only
    balanced = rain[...] - mean_fresh
    virtual = -surface[0] * balanced + total_salt / total_area
    wet = (sea[...] > 0).astype(jnp.float32)
    out[0] = salt_next[0] + time_step / top_thickness * virtual * wet


def add_virtual(salt_next, brine, rain, sea, totals):
    levels, rows, width = salt_next.shape
    plane = pl.BlockSpec((rows, width), lambda i: (0, 0))
    top = pl.BlockSpec((1, rows, width), lambda i: (0, 0, 0))
    return pl.pallas_call(
        final_kernel,
        grid=(1,),
        in_specs=[top, top, plane, plane, pl.BlockSpec((1, LANES), lambda i: (0, 0))],
        out_specs=top,
        out_shape=jax.ShapeDtypeStruct(salt_next.shape, jnp.float32),
        input_output_aliases={0: 0},
        name="add_virtual",
    )(salt_next, brine, rain, sea, totals)


def all_sum(vector, axis):
    count = lax.axis_size(axis)
    copies = jnp.broadcast_to(vector[None], (count,) + vector.shape)
    return jnp.sum(lax.all_to_all(copies, axis, 0, 0, tiled=True), axis=0)


def along(block, axis, by, closed):
    count = lax.axis_size(axis)
    pairs = [(i, (i + by) % count) for i in range(count) if closed or i + by in range(count)]
    return lax.ppermute(block, axis, pairs)


def fold_exchange(rows, seam, width):
    around, height = lax.axis_size("gx"), lax.axis_size("gy")
    centre = (seam[0] // width + lax.axis_index("gx")) % around

    def branch(middle):
        pairs = [
            (i * height + height - 1, (middle - i) % around * height + height - 1) for i in range(around)
        ]
        return lambda block: lax.ppermute(block, ("gx", "gy"), pairs)

    return lax.switch(centre, [branch(middle) for middle in range(around)], rows)


def shards(heat, brine, currents, sea, layers, area, rain, seam):
    levels, rows, width = heat.shape
    sums = local_sums(brine, sea, area, rain)
    west_own, east_own, south_own, north_own, fold_own = packs(heat, brine, currents, sea, layers)
    totals = all_sum(all_sum(sums, "gx"), "gy")
    west_halo = along(east_own, "gx", 1, True)
    east_halo = along(west_own, "gx", -1, True)
    south_halo = along(north_own, "gy", 1, False)
    north_halo = along(south_own, "gy", -1, False)
    fold_halo = fold_exchange(fold_own, seam, width)
    is_top = (lax.axis_index("gy") == lax.axis_size("gy") - 1).astype(jnp.int32)
    heat_next, salt_next = pl.pallas_call(
        step_kernel,
        in_specs=[pl.BlockSpec(memory_space=pltpu.SMEM)] + [VMEM] * 13,
        out_specs=[VMEM] * 2,
        out_shape=[jax.ShapeDtypeStruct(heat.shape, jnp.float32)] * 2,
        name="tracer_step",
    )(
        is_top[None], heat, brine, currents, sea, layers, area,
        west_own, east_own, west_halo, east_halo, south_halo, north_halo, fold_halo,
    )
    return heat_next, add_virtual(salt_next, brine, rain, sea, totals)


def solution(mesh):
    cells = P("groups", "gy", "gx")
    plane = P("gy", "gx")
    in_specs = (cells, cells, P("groups", None, "gy", "gx"), plane, plane, plane, plane, P("gx"))
    return jax.shard_map(
        shards, mesh=mesh, in_specs=in_specs, out_specs=(cells, cells), check_vma=False
    )
```

```python
import math

import jax
import jax.numpy as jnp
from jax import lax
from jax.experimental import pallas as pl
from jax.experimental.pallas import tpu as pltpu
from jax.sharding import PartitionSpec as P

time_step = 0.25
diffusivity = 0.5
vertical_mixing = 0.3
top_thickness = 0.5

VMEM = pl.BlockSpec(memory_space=pltpu.VMEM)
LANES = 128


def lane_of(shape):
    return lax.broadcasted_iota(jnp.int32, shape, len(shape) - 1)


def sums_kernel(surface, sea, area, rain, out):
    wet_area = area[...] * sea[...].astype(jnp.float32)
    salt = wet_area * surface[0]
    rain_now = rain[...]
    lane = lane_of((1, LANES))
    packed = jnp.zeros((1, LANES), jnp.float32)
    for place, field in enumerate((wet_area, wet_area * rain_now, salt * rain_now, salt)):
        total = jnp.sum(jnp.sum(field, axis=0, keepdims=True), axis=1, keepdims=True)
        packed = jnp.where(lane == place, total, packed)
    out[...] = packed


def local_sums(brine, sea, area, rain):
    rows, width = sea.shape
    plane = pl.BlockSpec((rows, width), lambda i: (0, 0))
    return pl.pallas_call(
        sums_kernel,
        grid=(1,),
        in_specs=[pl.BlockSpec((1, rows, width), lambda i: (0, 0, 0)), plane, plane, plane],
        out_specs=pl.BlockSpec((1, LANES), lambda i: (0, 0)),
        out_shape=jax.ShapeDtypeStruct((1, LANES), jnp.float32),
        name="local_sums",
    )(brine, sea, area, rain)


def mirrored(rows):
    lane = lane_of(rows.shape)
    bit = 1
    while bit < LANES:
        low = (lane // bit) % 2 == 0
        rows = jnp.where(low, pltpu.roll(rows, LANES - bit, 1), pltpu.roll(rows, bit, 1))
        bit *= 2
    return rows


def column_pack(planes, lane_number):
    lane = lane_of((8, LANES))
    blocks = planes[0].shape[0] // 8
    packed = jnp.zeros((8, LANES), jnp.float32)
    for level, plane in enumerate(planes):
        for block in range(blocks):
            place = level * blocks + block
            tile = plane[8 * block : 8 * block + 8]
            moved = pltpu.roll(tile, (place - lane_number) % LANES, 1)
            packed = jnp.where(lane == place, moved, packed)
    return packed


def pack_kernel(heat, salt, currents, sea, layers, west, east, south, north, fold):
    levels, rows, _ = heat.shape
    depth = (sea[...] * layers[...]).astype(jnp.float32)
    heat_planes = [heat[k] for k in range(levels)]
    salt_planes = [salt[k] for k in range(levels)]
    speed_planes = [currents[0, k] for k in range(levels)]
    depth_planes = [depth] * levels
    west[0:8] = column_pack(heat_planes, 0)
    west[8:16] = column_pack(salt_planes, 0)
    west[16:24] = column_pack(depth_planes, 0)
    east[0:8] = column_pack(heat_planes, LANES - 1)
    east[8:16] = column_pack(salt_planes, LANES - 1)
    east[16:24] = column_pack(depth_planes, LANES - 1)
    east[24:32] = column_pack(speed_planes, LANES - 1)
    last = rows - 1
    for k in range(levels):
        south[k : k + 1] = heat[k, 0:1]
        south[levels + k : levels + k + 1] = salt[k, 0:1]
        north[k : k + 1] = heat[k, last:rows]
        north[levels + k : levels + k + 1] = salt[k, last:rows]
        north[2 * levels + 8 + k : 2 * levels + 9 + k] = currents[1, k, last:rows]
    south[2 * levels : 2 * levels + 8] = jnp.broadcast_to(depth[0:1], (8, LANES))
    north[2 * levels : 2 * levels + 8] = jnp.broadcast_to(depth[last:rows], (8, LANES))
    fold[...] = mirrored(north[...])


def packs(heat, salt, currents, sea, layers):
    levels, rows, width = heat.shape
    shapes = (24, 32, 2 * levels + 8, 3 * levels + 8, 3 * levels + 8)
    return pl.pallas_call(
        pack_kernel,
        in_specs=[VMEM] * 5,
        out_specs=[VMEM] * 5,
        out_shape=[jax.ShapeDtypeStruct((n, LANES), jnp.float32) for n in shapes],
        name="edge_packs",
    )(heat, salt, currents, sea, layers)


def open_flux(near, far, forward, backward):
    return forward * near + backward * far - diffusivity * (far - near)


def edge_flux(near, far, speed, near_depth, far_depth, level):
    wet = (level < jnp.minimum(near_depth, far_depth)).astype(jnp.float32)
    return wet * open_flux(near, far, jnp.maximum(speed, 0.0), jnp.minimum(speed, 0.0))


def step_kernel(
    flags, heat, salt, currents, sea, layers, area,
    west_own, east_own, west_halo, east_halo, south_halo, north_halo, fold_halo,
    heat_out, salt_out,
):
    levels, rows, _ = heat.shape
    blocks = rows // 8
    lane = lane_of((rows, LANES))
    row = lax.broadcasted_iota(jnp.int32, (rows, LANES), 0)
    first_lane, last_lane = lane == 0, lane == LANES - 1
    first_row, last_row = row == 0, row == rows - 1
    is_top = flags[0] == 1
    depth = (sea[...] * layers[...]).astype(jnp.float32)
    base = 2 * levels
    north_depth = jnp.where(is_top, fold_halo[base : base + 1], north_halo[base : base + 1])
    south_depth = south_halo[base : base + 1]
    depth_north = jnp.where(last_row, north_depth, pltpu.roll(depth, rows - 1, 0))
    open_north = jnp.minimum(depth, depth_north)
    open_south = jnp.minimum(depth[0:1], south_depth)
    open_east = jnp.where(last_lane, 0.0, jnp.minimum(depth, pltpu.roll(depth, LANES - 1, 1)))
    per_area = time_step / area[...]
    edge_level = (lane_of((8, LANES)) // blocks).astype(jnp.float32)
    west_edge, east_edge = [], []
    for f in range(2):
        own_west, own_east = west_own[8 * f : 8 * f + 8], east_own[8 * f : 8 * f + 8]
        west_edge.append(
            edge_flux(west_halo[8 * f : 8 * f + 8], own_west, west_halo[24:32], west_halo[16:24], west_own[16:24], edge_level)
        )
        east_edge.append(
            edge_flux(own_east, east_halo[8 * f : 8 * f + 8], east_own[24:32], east_own[16:24], east_halo[16:24], edge_level)
        )
    fields = (heat, salt)
    above = [None, None]
    for k in range(levels):
        level = float(k)
        east_speed = currents[0, k]
        north_speed = currents[1, k]
        fold_speed = 0.5 * (north_speed[rows - 1 : rows] - fold_halo[base + 8 + k : base + 9 + k])
        top_speed = jnp.where(is_top, fold_speed, north_speed[rows - 1 : rows])
        north_speed = jnp.where(last_row, top_speed, north_speed)
        south_speed = south_halo[base + 8 + k : base + 9 + k]
        east_up, east_down = jnp.maximum(east_speed, 0.0), jnp.minimum(east_speed, 0.0)
        north_up, north_down = jnp.maximum(north_speed, 0.0), jnp.minimum(north_speed, 0.0)
        east_wet = level < open_east
        north_wet = level < open_north
        for f in range(2):
            cells = fields[f][k]
            at = f * levels + k
            east_flux = jnp.where(
                east_wet, open_flux(cells, pltpu.roll(cells, LANES - 1, 1), east_up, east_down), 0.0
            )
            west_flux = pltpu.roll(east_flux, 1, 1)
            west_columns, east_columns = [], []
            for block in range(blocks):
                place = k * blocks + block
                west_columns.append(pltpu.roll(west_edge[f], (-place) % LANES, 1))
                east_columns.append(pltpu.roll(east_edge[f], (LANES - 1 - place) % LANES, 1))
            west_flux = jnp.where(first_lane, jnp.concatenate(west_columns, axis=0), west_flux)
            east_flux = jnp.where(last_lane, jnp.concatenate(east_columns, axis=0), east_flux)
            top_cells = jnp.where(is_top, fold_halo[at : at + 1], north_halo[at : at + 1])
            northern = jnp.where(last_row, top_cells, pltpu.roll(cells, rows - 1, 0))
            north_flux = jnp.where(north_wet, open_flux(cells, northern, north_up, north_down), 0.0)
            first_flux = edge_flux(south_halo[at : at + 1], cells[0:1], south_speed, open_south, open_south, level)
            south_flux = jnp.where(first_row, first_flux, pltpu.roll(north_flux, 1, 0))
            change = per_area * (west_flux - east_flux + south_flux - north_flux)
            if k > 0:
                change = change + time_step * above[f]
            if k < levels - 1:
                below = jnp.where(level + 1.0 < depth, vertical_mixing * (cells - fields[f][k + 1]), 0.0)
                change = change - time_step * below
                above[f] = below
            result = cells + jnp.where(level < depth, change, 0.0)
            (heat_out, salt_out)[f][k] = result


def final_kernel(salt_next, surface, rain, sea, totals, out):
    lane = lane_of((1, LANES))

    def total(place):
        return jnp.sum(jnp.where(lane == place, totals[...], 0.0), axis=1, keepdims=True)

    total_area, total_fresh, salt_fresh, salt_only = (total(place) for place in range(4))
    mean_fresh = total_fresh / total_area
    total_salt = salt_fresh - mean_fresh * salt_only
    balanced = rain[...] - mean_fresh
    virtual = -surface[0] * balanced + total_salt / total_area
    wet = (sea[...] > 0).astype(jnp.float32)
    out[0] = salt_next[0] + time_step / top_thickness * virtual * wet


def add_virtual(salt_next, brine, rain, sea, totals):
    levels, rows, width = salt_next.shape
    plane = pl.BlockSpec((rows, width), lambda i: (0, 0))
    top = pl.BlockSpec((1, rows, width), lambda i: (0, 0, 0))
    return pl.pallas_call(
        final_kernel,
        grid=(1,),
        in_specs=[top, top, plane, plane, pl.BlockSpec((1, LANES), lambda i: (0, 0))],
        out_specs=top,
        out_shape=jax.ShapeDtypeStruct(salt_next.shape, jnp.float32),
        input_output_aliases={0: 0},
        name="add_virtual",
    )(salt_next, brine, rain, sea, totals)


def all_sum(vector, axis):
    count = lax.axis_size(axis)
    copies = jnp.broadcast_to(vector[None], (count,) + vector.shape)
    return jnp.sum(lax.all_to_all(copies, axis, 0, 0, tiled=True), axis=0)


def along(block, axis, by, closed):
    count = lax.axis_size(axis)
    pairs = [(i, (i + by) % count) for i in range(count) if closed or i + by in range(count)]
    return lax.ppermute(block, axis, pairs)


def fold_exchange(rows, seam, width):
    around, height = lax.axis_size("gx"), lax.axis_size("gy")
    radix = max(1, math.isqrt(around))
    centre = (seam[0] // width + lax.axis_index("gx")) % around

    def top_permute(target):
        pairs = [(i * height + height - 1, target(i) % around * height + height - 1) for i in range(around)]
        return lambda block: lax.ppermute(block, ("gx", "gy"), pairs)

    def mirror(coarse):
        return top_permute(lambda i: coarse * radix + radix // 2 - i)

    def shift(fine):
        return top_permute(lambda i: i + fine - radix // 2)

    rows = lax.switch(centre // radix, [mirror(coarse) for coarse in range(-(-around // radix))], rows)
    return lax.switch(centre % radix, [shift(fine) for fine in range(radix)], rows)


def shards(heat, brine, currents, sea, layers, area, rain, seam):
    levels, rows, width = heat.shape
    sums = local_sums(brine, sea, area, rain)
    west_own, east_own, south_own, north_own, fold_own = packs(heat, brine, currents, sea, layers)
    totals = all_sum(all_sum(sums, "gx"), "gy")
    west_halo = along(east_own, "gx", 1, True)
    east_halo = along(west_own, "gx", -1, True)
    south_halo = along(north_own, "gy", 1, False)
    north_halo = along(south_own, "gy", -1, False)
    fold_halo = fold_exchange(fold_own, seam, width)
    is_top = (lax.axis_index("gy") == lax.axis_size("gy") - 1).astype(jnp.int32)
    heat_next, salt_next = pl.pallas_call(
        step_kernel,
        in_specs=[pl.BlockSpec(memory_space=pltpu.SMEM)] + [VMEM] * 13,
        out_specs=[VMEM] * 2,
        out_shape=[jax.ShapeDtypeStruct(heat.shape, jnp.float32)] * 2,
        name="tracer_step",
    )(
        is_top[None], heat, brine, currents, sea, layers, area,
        west_own, east_own, west_halo, east_halo, south_halo, north_halo, fold_halo,
    )
    return heat_next, add_virtual(salt_next, brine, rain, sea, totals)


def solution(mesh):
    cells = P("groups", "gy", "gx")
    plane = P("gy", "gx")
    in_specs = (cells, cells, P("groups", None, "gy", "gx"), plane, plane, plane, plane, P("gx"))
    return jax.shard_map(
        shards, mesh=mesh, in_specs=in_specs, out_specs=(cells, cells), check_vma=False
    )
```

```python
import jax
import jax.numpy as jnp
from jax import lax
from jax.experimental import pallas as pl
from jax.experimental.pallas import tpu as pltpu
from jax.sharding import PartitionSpec as P

time_step = 0.25
diffusivity = 0.5
vertical_mixing = 0.3
top_thickness = 0.5

VMEM = pl.BlockSpec(memory_space=pltpu.VMEM)
LANES = 128


def lane_of(shape):
    return lax.broadcasted_iota(jnp.int32, shape, len(shape) - 1)


def sums_kernel(surface, sea, area, rain, out):
    wet_area = area[...] * sea[...].astype(jnp.float32)
    salt = wet_area * surface[0]
    rain_now = rain[...]
    lane = lane_of((1, LANES))
    packed = jnp.zeros((1, LANES), jnp.float32)
    for place, field in enumerate((wet_area, wet_area * rain_now, salt * rain_now, salt)):
        total = jnp.sum(jnp.sum(field, axis=0, keepdims=True), axis=1, keepdims=True)
        packed = jnp.where(lane == place, total, packed)
    out[...] = jnp.broadcast_to(packed[None], out.shape)


def local_sums(brine, sea, area, rain, copies):
    rows, width = sea.shape
    plane = pl.BlockSpec((rows, width), lambda i: (0, 0))
    return pl.pallas_call(
        sums_kernel,
        grid=(1,),
        in_specs=[pl.BlockSpec((1, rows, width), lambda i: (0, 0, 0)), plane, plane, plane],
        out_specs=pl.BlockSpec((copies, 1, LANES), lambda i: (0, 0, 0)),
        out_shape=jax.ShapeDtypeStruct((copies, 1, LANES), jnp.float32),
        name="local_sums",
    )(brine, sea, area, rain)


def mirrored(rows):
    lane = lane_of(rows.shape)
    bit = 1
    while bit < LANES:
        low = (lane // bit) % 2 == 0
        rows = jnp.where(low, pltpu.roll(rows, LANES - bit, 1), pltpu.roll(rows, bit, 1))
        bit *= 2
    return rows


def column_pack(planes, lane_number):
    lane = lane_of((8, LANES))
    blocks = planes[0].shape[0] // 8
    packed = jnp.zeros((8, LANES), jnp.float32)
    for level, plane in enumerate(planes):
        for block in range(blocks):
            place = level * blocks + block
            tile = plane[8 * block : 8 * block + 8]
            moved = pltpu.roll(tile, (place - lane_number) % LANES, 1)
            packed = jnp.where(lane == place, moved, packed)
    return packed


def pack_kernel(heat, salt, currents, sea, layers, west, east, south, north, fold):
    levels, rows, _ = heat.shape
    depth = (sea[...] * layers[...]).astype(jnp.float32)
    heat_planes = [heat[k] for k in range(levels)]
    salt_planes = [salt[k] for k in range(levels)]
    speed_planes = [currents[0, k] for k in range(levels)]
    depth_planes = [depth] * levels
    west[0:8] = column_pack(heat_planes, 0)
    west[8:16] = column_pack(salt_planes, 0)
    west[16:24] = column_pack(depth_planes, 0)
    east[0:8] = column_pack(heat_planes, LANES - 1)
    east[8:16] = column_pack(salt_planes, LANES - 1)
    east[16:24] = column_pack(depth_planes, LANES - 1)
    east[24:32] = column_pack(speed_planes, LANES - 1)
    last = rows - 1
    for k in range(levels):
        south[k : k + 1] = heat[k, 0:1]
        south[levels + k : levels + k + 1] = salt[k, 0:1]
        north[k : k + 1] = heat[k, last:rows]
        north[levels + k : levels + k + 1] = salt[k, last:rows]
        north[2 * levels + 8 + k : 2 * levels + 9 + k] = currents[1, k, last:rows]
    south[2 * levels : 2 * levels + 8] = jnp.broadcast_to(depth[0:1], (8, LANES))
    north[2 * levels : 2 * levels + 8] = jnp.broadcast_to(depth[last:rows], (8, LANES))
    turned = mirrored(north[...])
    fold[...] = turned
    west[24:] = turned
    east[32:] = turned


def packs(heat, salt, currents, sea, layers):
    levels, rows, width = heat.shape
    north = 3 * levels + 8
    shapes = (24 + north, 32 + north, 2 * levels + 8, north, north)
    return pl.pallas_call(
        pack_kernel,
        in_specs=[VMEM] * 5,
        out_specs=[VMEM] * 5,
        out_shape=[jax.ShapeDtypeStruct((n, LANES), jnp.float32) for n in shapes],
        name="edge_packs",
    )(heat, salt, currents, sea, layers)


def open_flux(near, far, forward, backward):
    return forward * near + backward * far - diffusivity * (far - near)


def edge_flux(near, far, speed, near_depth, far_depth, level):
    wet = (level < jnp.minimum(near_depth, far_depth)).astype(jnp.float32)
    return wet * open_flux(near, far, jnp.maximum(speed, 0.0), jnp.minimum(speed, 0.0))


def step_kernel(
    heat, salt, currents, sea, layers, area,
    west_own, east_own, west_halo, east_halo, south_halo, north_halo,
    heat_out, salt_out,
):
    levels, rows, _ = heat.shape
    blocks = rows // 8
    lane = lane_of((rows, LANES))
    row = lax.broadcasted_iota(jnp.int32, (rows, LANES), 0)
    first_lane, last_lane = lane == 0, lane == LANES - 1
    first_row, last_row = row == 0, row == rows - 1
    depth = (sea[...] * layers[...]).astype(jnp.float32)
    base = 2 * levels
    south_depth = south_halo[base : base + 1]
    depth_north = jnp.where(last_row, north_halo[base : base + 1], pltpu.roll(depth, rows - 1, 0))
    open_north = jnp.minimum(depth, depth_north)
    open_south = jnp.minimum(depth[0:1], south_depth)
    open_east = jnp.where(last_lane, 0.0, jnp.minimum(depth, pltpu.roll(depth, LANES - 1, 1)))
    per_area = time_step / area[...]
    edge_level = (lane_of((8, LANES)) // blocks).astype(jnp.float32)
    west_edge, east_edge = [], []
    for f in range(2):
        own_west, own_east = west_own[8 * f : 8 * f + 8], east_own[8 * f : 8 * f + 8]
        west_edge.append(
            edge_flux(west_halo[8 * f : 8 * f + 8], own_west, west_halo[24:32], west_halo[16:24], west_own[16:24], edge_level)
        )
        east_edge.append(
            edge_flux(own_east, east_halo[8 * f : 8 * f + 8], east_own[24:32], east_own[16:24], east_halo[16:24], edge_level)
        )
    fields = (heat, salt)

    def one_level(k, above):
        level = k.astype(jnp.float32)
        east_speed, north_speed = currents[0, k], currents[1, k]
        south_speed = south_halo[pl.ds(base + 8 + k, 1)]
        east_up, east_down = jnp.maximum(east_speed, 0.0), jnp.minimum(east_speed, 0.0)
        north_up, north_down = jnp.maximum(north_speed, 0.0), jnp.minimum(north_speed, 0.0)
        east_wet = level < open_east
        north_wet = level < open_north
        wet = level < depth
        below_wet = level + 1.0 < depth
        passed = []
        for f in range(2):
            cells = fields[f][k]
            at = f * levels + k
            east_flux = jnp.where(
                east_wet, open_flux(cells, pltpu.roll(cells, LANES - 1, 1), east_up, east_down), 0.0
            )
            west_flux = pltpu.roll(east_flux, 1, 1)
            west_columns, east_columns = [], []
            for block in range(blocks):
                place = k * blocks + block
                west_columns.append(pltpu.roll(west_edge[f], (LANES - place) % LANES, 1))
                east_columns.append(pltpu.roll(east_edge[f], LANES - 1 - place, 1))
            west_flux = jnp.where(first_lane, jnp.concatenate(west_columns, axis=0), west_flux)
            east_flux = jnp.where(last_lane, jnp.concatenate(east_columns, axis=0), east_flux)
            northern = jnp.where(last_row, north_halo[pl.ds(at, 1)], pltpu.roll(cells, rows - 1, 0))
            north_flux = jnp.where(north_wet, open_flux(cells, northern, north_up, north_down), 0.0)
            first_flux = edge_flux(
                south_halo[pl.ds(at, 1)], cells[0:1], south_speed, open_south, open_south, level
            )
            south_flux = jnp.where(first_row, first_flux, pltpu.roll(north_flux, 1, 0))
            next_cells = fields[f][jnp.minimum(k + 1, levels - 1)]
            below = jnp.where(below_wet, vertical_mixing * (cells - next_cells), 0.0)
            change = per_area * (west_flux - east_flux + south_flux - north_flux) + time_step * (above[f] - below)
            (heat_out, salt_out)[f][k] = cells + jnp.where(wet, change, 0.0)
            passed.append(below)
        return tuple(passed)

    nothing = jnp.zeros((rows, LANES), jnp.float32)
    lax.fori_loop(0, levels, one_level, (nothing, nothing))


def tracer_step(*arrays):
    heat = arrays[0]
    return pl.pallas_call(
        step_kernel,
        in_specs=[VMEM] * 12,
        out_specs=[VMEM] * 2,
        out_shape=[jax.ShapeDtypeStruct(heat.shape, jnp.float32)] * 2,
        name="tracer_step",
    )(*arrays)


def fold_kernel(heat_next, salt_next, own, fold, area, heat_out, salt_out):
    levels, band, _ = heat_next.shape
    base = 2 * levels
    level = lax.broadcasted_iota(jnp.int32, (levels, LANES), 0).astype(jnp.float32)
    per_area = time_step / area[band - 1 : band]
    speed = 0.5 * (own[base + 8 :] - fold[base + 8 :])
    last = lax.broadcasted_iota(jnp.int32, (band, LANES), 0) == band - 1
    for f, (before, after) in enumerate(((heat_next, heat_out), (salt_next, salt_out))):
        flux = edge_flux(
            own[f * levels : f * levels + levels], fold[f * levels : f * levels + levels], speed,
            own[base : base + 1], fold[base : base + 1], level,
        )
        leaving = per_area * flux
        for k in range(levels):
            after[k] = before[k] - jnp.where(last, leaving[k : k + 1], 0.0)


def close_fold(heat_next, salt_next, own, fold, area):
    levels, rows, width = heat_next.shape
    band = pl.BlockSpec((levels, 8, width), lambda i: (0, rows // 8 - 1, 0))
    whole = pl.BlockSpec(own.shape, lambda i: (0, 0))
    return pl.pallas_call(
        fold_kernel,
        grid=(1,),
        in_specs=[band, band, whole, whole, pl.BlockSpec((8, width), lambda i: (rows // 8 - 1, 0))],
        out_specs=[band, band],
        out_shape=[jax.ShapeDtypeStruct(heat_next.shape, jnp.float32)] * 2,
        input_output_aliases={0: 0, 1: 1},
        name="close_fold",
    )(heat_next, salt_next, own, fold, area)


def final_kernel(salt_next, surface, rain, sea, totals, out):
    lane = lane_of((1, LANES))

    def total(place):
        return jnp.sum(jnp.where(lane == place, totals[...], 0.0), axis=1, keepdims=True)

    total_area, total_fresh, salt_fresh, salt_only = (total(place) for place in range(4))
    mean_fresh = total_fresh / total_area
    total_salt = salt_fresh - mean_fresh * salt_only
    balanced = rain[...] - mean_fresh
    virtual = -surface[0] * balanced + total_salt / total_area
    wet = (sea[...] > 0).astype(jnp.float32)
    out[0] = salt_next[0] + time_step / top_thickness * virtual * wet


def add_virtual(salt_next, brine, rain, sea, totals):
    levels, rows, width = salt_next.shape
    plane = pl.BlockSpec((rows, width), lambda i: (0, 0))
    top = pl.BlockSpec((1, rows, width), lambda i: (0, 0, 0))
    return pl.pallas_call(
        final_kernel,
        grid=(1,),
        in_specs=[top, top, plane, plane, pl.BlockSpec((1, LANES), lambda i: (0, 0))],
        out_specs=top,
        out_shape=jax.ShapeDtypeStruct(salt_next.shape, jnp.float32),
        input_output_aliases={0: 0},
        name="add_virtual",
    )(salt_next, brine, rain, sea, totals)


def all_sum(copies, axis):
    return jnp.sum(lax.all_to_all(copies, axis, 0, 0, tiled=True), axis=0)


def along(block, axis, by, closed):
    count = lax.axis_size(axis)
    pairs = [(i, (i + by) % count) for i in range(count) if closed or i + by in range(count)]
    return lax.ppermute(block, axis, pairs)


def fold_exchange(own, from_west, from_east, seam, width, beside):
    around, height = lax.axis_size("gx"), lax.axis_size("gy")
    centre = (seam[0] // width + lax.axis_index("gx")) % around
    part = (centre + 1) % 3
    held = jnp.where(part == 0, from_west, jnp.where(part == 2, from_east, own))

    def mirror(coarse):
        pairs = [
            (i * height + height - 1, (3 * coarse - i) % around * height + height - 1) for i in range(around)
        ]

        def branch(rows, arrays):
            return lax.ppermute(rows, ("gx", "gy"), pairs), beside(*arrays)

        return branch

    return (centre + 1) // 3, [mirror(coarse) for coarse in range((around + 2) // 3)], held


def shards(heat, brine, currents, sea, layers, area, rain, seam):
    levels, rows, width = heat.shape
    sums = local_sums(brine, sea, area, rain, lax.axis_size("gx"))
    row_totals = all_sum(sums, "gx")
    west_own, east_own, south_own, north_own, fold_own = packs(heat, brine, currents, sea, layers)
    west_halo = along(east_own, "gx", 1, True)
    east_halo = along(west_own, "gx", -1, True)
    south_halo = along(north_own, "gy", 1, False)
    north_halo = along(south_own, "gy", -1, False)
    place, branches, held = fold_exchange(fold_own, west_halo[32:], east_halo[24:], seam, width, tracer_step)
    arrays = (
        heat, brine, currents, sea, layers, area,
        west_own, east_own, west_halo, east_halo, south_halo, north_halo,
    )
    fold_halo, (heat_next, salt_next) = lax.switch(place, branches, held, arrays)
    row_totals, fold_halo = lax.optimization_barrier((row_totals, fold_halo))
    height = lax.axis_size("gy")
    totals = all_sum(jnp.broadcast_to(row_totals[None], (height,) + row_totals.shape), "gy")
    heat_next, salt_next = close_fold(heat_next, salt_next, north_own, fold_halo, area)
    return heat_next, add_virtual(salt_next, brine, rain, sea, totals)


def solution(mesh):
    cells = P("groups", "gy", "gx")
    plane = P("gy", "gx")
    in_specs = (cells, cells, P("groups", None, "gy", "gx"), plane, plane, plane, plane, P("gx"))
    return jax.shard_map(
        shards, mesh=mesh, in_specs=in_specs, out_specs=(cells, cells), check_vma=False
    )
```

```python
import jax
import jax.numpy as jnp
from jax import lax
from jax.experimental import pallas as pl
from jax.experimental.pallas import tpu as pltpu
from jax.sharding import Mesh
from jax.sharding import PartitionSpec as P

time_step = 0.25
diffusivity = 0.5
vertical_mixing = 0.3
top_thickness = 0.5

VMEM = pl.BlockSpec(memory_space=pltpu.VMEM)
LANES = 128
CORES = 2
GX = ("chip", "core")
NEAR = ("core", "gy")


def lane_of(shape):
    return lax.broadcasted_iota(jnp.int32, shape, len(shape) - 1)


def sums_kernel(surface, sea, area, rain, out):
    wet_area = area[...] * sea[...].astype(jnp.float32)
    salt = wet_area * surface[0]
    rain_now = rain[...]
    lane = lane_of((1, LANES))
    packed = jnp.zeros((1, LANES), jnp.float32)
    for place, field in enumerate((wet_area, wet_area * rain_now, salt * rain_now, salt)):
        total = jnp.sum(jnp.sum(field, axis=0, keepdims=True), axis=1, keepdims=True)
        packed = jnp.where(lane == place, total, packed)
    out[...] = jnp.broadcast_to(packed[None], out.shape)


def local_sums(brine, sea, area, rain, copies):
    rows, width = sea.shape
    plane = pl.BlockSpec((rows, width), lambda i: (0, 0))
    return pl.pallas_call(
        sums_kernel,
        grid=(1,),
        in_specs=[pl.BlockSpec((1, rows, width), lambda i: (0, 0, 0)), plane, plane, plane],
        out_specs=pl.BlockSpec((copies, 1, LANES), lambda i: (0, 0, 0)),
        out_shape=jax.ShapeDtypeStruct((copies, 1, LANES), jnp.float32),
        name="local_sums",
    )(brine, sea, area, rain)


def mirrored(rows):
    lane = lane_of(rows.shape)
    bit = 1
    while bit < LANES:
        low = (lane // bit) % 2 == 0
        rows = jnp.where(low, pltpu.roll(rows, LANES - bit, 1), pltpu.roll(rows, bit, 1))
        bit *= 2
    return rows


def column_pack(planes, lane_number):
    lane = lane_of((8, LANES))
    blocks = planes[0].shape[0] // 8
    packed = jnp.zeros((8, LANES), jnp.float32)
    for level, plane in enumerate(planes):
        for block in range(blocks):
            place = level * blocks + block
            tile = plane[8 * block : 8 * block + 8]
            moved = pltpu.roll(tile, (place - lane_number) % LANES, 1)
            packed = jnp.where(lane == place, moved, packed)
    return packed


def pack_kernel(heat, salt, currents, sea, layers, west, east, south, north, fold):
    levels, rows, _ = heat.shape
    depth = (sea[...] * layers[...]).astype(jnp.float32)
    heat_planes = [heat[k] for k in range(levels)]
    salt_planes = [salt[k] for k in range(levels)]
    speed_planes = [currents[0, k] for k in range(levels)]
    depth_planes = [depth] * levels
    west[0:8] = column_pack(heat_planes, 0)
    west[8:16] = column_pack(salt_planes, 0)
    west[16:24] = column_pack(depth_planes, 0)
    east[0:8] = column_pack(heat_planes, LANES - 1)
    east[8:16] = column_pack(salt_planes, LANES - 1)
    east[16:24] = column_pack(depth_planes, LANES - 1)
    east[24:32] = column_pack(speed_planes, LANES - 1)
    last = rows - 1
    for k in range(levels):
        south[k : k + 1] = heat[k, 0:1]
        south[levels + k : levels + k + 1] = salt[k, 0:1]
        north[k : k + 1] = heat[k, last:rows]
        north[levels + k : levels + k + 1] = salt[k, last:rows]
        north[2 * levels + 8 + k : 2 * levels + 9 + k] = currents[1, k, last:rows]
    south[2 * levels : 2 * levels + 8] = jnp.broadcast_to(depth[0:1], (8, LANES))
    north[2 * levels : 2 * levels + 8] = jnp.broadcast_to(depth[last:rows], (8, LANES))
    turned = mirrored(north[...])
    fold[...] = turned
    west[24:] = turned
    east[32:] = turned


def packs(heat, salt, currents, sea, layers):
    levels, _, _ = heat.shape
    north = 3 * levels + 8
    shapes = (24 + north, 32 + north, 2 * levels + 8, north, north)
    return pl.pallas_call(
        pack_kernel,
        in_specs=[VMEM] * 5,
        out_specs=[VMEM] * 5,
        out_shape=[jax.ShapeDtypeStruct((n, LANES), jnp.float32) for n in shapes],
        name="edge_packs",
    )(heat, salt, currents, sea, layers)


def open_flux(near, far, forward, backward):
    return forward * near + backward * far - diffusivity * (far - near)


def edge_flux(near, far, speed, near_depth, far_depth, level):
    wet = (level < jnp.minimum(near_depth, far_depth)).astype(jnp.float32)
    return wet * open_flux(near, far, jnp.maximum(speed, 0.0), jnp.minimum(speed, 0.0))


def step_kernel(
    heat, salt, currents, sea, layers, area,
    west_own, east_own, west_halo, east_halo, south_halo, north_halo,
    heat_out, salt_out,
):
    levels, rows, _ = heat.shape
    blocks = rows // 8
    lane = lane_of((rows, LANES))
    row = lax.broadcasted_iota(jnp.int32, (rows, LANES), 0)
    first_lane, last_lane = lane == 0, lane == LANES - 1
    first_row, last_row = row == 0, row == rows - 1
    depth = (sea[...] * layers[...]).astype(jnp.float32)
    base = 2 * levels
    south_depth = south_halo[base : base + 1]
    depth_north = jnp.where(last_row, north_halo[base : base + 1], pltpu.roll(depth, rows - 1, 0))
    open_north = jnp.minimum(depth, depth_north)
    open_south = jnp.minimum(depth[0:1], south_depth)
    open_east = jnp.where(last_lane, 0.0, jnp.minimum(depth, pltpu.roll(depth, LANES - 1, 1)))
    per_area = time_step / area[...]
    edge_level = (lane_of((8, LANES)) // blocks).astype(jnp.float32)
    west_edge, east_edge = [], []
    for f in range(2):
        own_west, own_east = west_own[8 * f : 8 * f + 8], east_own[8 * f : 8 * f + 8]
        west_edge.append(
            edge_flux(west_halo[8 * f : 8 * f + 8], own_west, west_halo[24:32], west_halo[16:24], west_own[16:24], edge_level)
        )
        east_edge.append(
            edge_flux(own_east, east_halo[8 * f : 8 * f + 8], east_own[24:32], east_own[16:24], east_halo[16:24], edge_level)
        )
    fields = (heat, salt)

    def one_level(k, above):
        level = k.astype(jnp.float32)
        east_speed, north_speed = currents[0, k], currents[1, k]
        south_speed = south_halo[pl.ds(base + 8 + k, 1)]
        east_up, east_down = jnp.maximum(east_speed, 0.0), jnp.minimum(east_speed, 0.0)
        north_up, north_down = jnp.maximum(north_speed, 0.0), jnp.minimum(north_speed, 0.0)
        east_wet = level < open_east
        north_wet = level < open_north
        wet = level < depth
        below_wet = level + 1.0 < depth
        passed = []
        for f in range(2):
            cells = fields[f][k]
            at = f * levels + k
            east_flux = jnp.where(
                east_wet, open_flux(cells, pltpu.roll(cells, LANES - 1, 1), east_up, east_down), 0.0
            )
            west_flux = pltpu.roll(east_flux, 1, 1)
            west_columns, east_columns = [], []
            for block in range(blocks):
                place = k * blocks + block
                west_columns.append(pltpu.roll(west_edge[f], (LANES - place) % LANES, 1))
                east_columns.append(pltpu.roll(east_edge[f], LANES - 1 - place, 1))
            west_flux = jnp.where(first_lane, jnp.concatenate(west_columns, axis=0), west_flux)
            east_flux = jnp.where(last_lane, jnp.concatenate(east_columns, axis=0), east_flux)
            northern = jnp.where(last_row, north_halo[pl.ds(at, 1)], pltpu.roll(cells, rows - 1, 0))
            north_flux = jnp.where(north_wet, open_flux(cells, northern, north_up, north_down), 0.0)
            first_flux = edge_flux(
                south_halo[pl.ds(at, 1)], cells[0:1], south_speed, open_south, open_south, level
            )
            south_flux = jnp.where(first_row, first_flux, pltpu.roll(north_flux, 1, 0))
            next_cells = fields[f][jnp.minimum(k + 1, levels - 1)]
            below = jnp.where(below_wet, vertical_mixing * (cells - next_cells), 0.0)
            change = per_area * (west_flux - east_flux + south_flux - north_flux) + time_step * (above[f] - below)
            (heat_out, salt_out)[f][k] = cells + jnp.where(wet, change, 0.0)
            passed.append(below)
        return tuple(passed)

    nothing = jnp.zeros((rows, LANES), jnp.float32)
    lax.fori_loop(0, levels, one_level, (nothing, nothing))


def tracer_step(*arrays):
    heat = arrays[0]
    return pl.pallas_call(
        step_kernel,
        in_specs=[VMEM] * 12,
        out_specs=[VMEM] * 2,
        out_shape=[jax.ShapeDtypeStruct(heat.shape, jnp.float32)] * 2,
        name="tracer_step",
    )(*arrays)


def fold_kernel(heat_next, salt_next, own, fold, area, heat_out, salt_out):
    levels, band, _ = heat_next.shape
    base = 2 * levels
    level = lax.broadcasted_iota(jnp.int32, (levels, LANES), 0).astype(jnp.float32)
    per_area = time_step / area[band - 1 : band]
    speed = 0.5 * (own[base + 8 :] - fold[base + 8 :])
    last = lax.broadcasted_iota(jnp.int32, (band, LANES), 0) == band - 1
    for f, (before, after) in enumerate(((heat_next, heat_out), (salt_next, salt_out))):
        flux = edge_flux(
            own[f * levels : f * levels + levels], fold[f * levels : f * levels + levels], speed,
            own[base : base + 1], fold[base : base + 1], level,
        )
        leaving = per_area * flux
        for k in range(levels):
            after[k] = before[k] - jnp.where(last, leaving[k : k + 1], 0.0)


def close_fold(heat_next, salt_next, own, fold, area):
    levels, rows, width = heat_next.shape
    band = pl.BlockSpec((levels, 8, width), lambda i: (0, rows // 8 - 1, 0))
    whole = pl.BlockSpec(own.shape, lambda i: (0, 0))
    return pl.pallas_call(
        fold_kernel,
        grid=(1,),
        in_specs=[band, band, whole, whole, pl.BlockSpec((8, width), lambda i: (rows // 8 - 1, 0))],
        out_specs=[band, band],
        out_shape=[jax.ShapeDtypeStruct(heat_next.shape, jnp.float32)] * 2,
        input_output_aliases={0: 0, 1: 1},
        name="close_fold",
    )(heat_next, salt_next, own, fold, area)


def final_kernel(salt_next, surface, rain, sea, totals, out):
    lane = lane_of((1, LANES))

    def total(place):
        return jnp.sum(jnp.where(lane == place, totals[...], 0.0), axis=1, keepdims=True)

    total_area, total_fresh, salt_fresh, salt_only = (total(place) for place in range(4))
    mean_fresh = total_fresh / total_area
    total_salt = salt_fresh - mean_fresh * salt_only
    balanced = rain[...] - mean_fresh
    virtual = -surface[0] * balanced + total_salt / total_area
    wet = (sea[...] > 0).astype(jnp.float32)
    out[0] = salt_next[0] + time_step / top_thickness * virtual * wet


def add_virtual(salt_next, brine, rain, sea, totals):
    _, rows, width = salt_next.shape
    plane = pl.BlockSpec((rows, width), lambda i: (0, 0))
    top = pl.BlockSpec((1, rows, width), lambda i: (0, 0, 0))
    return pl.pallas_call(
        final_kernel,
        grid=(1,),
        in_specs=[top, top, plane, plane, pl.BlockSpec((1, LANES), lambda i: (0, 0))],
        out_specs=top,
        out_shape=jax.ShapeDtypeStruct(salt_next.shape, jnp.float32),
        input_output_aliases={0: 0},
        name="add_virtual",
    )(salt_next, brine, rain, sea, totals)


def all_sum(copies, axes):
    return jnp.sum(lax.all_to_all(copies, axes, 0, 0, tiled=True), axis=0)


def along(block, axis, by, closed):
    count = lax.axis_size(axis)
    pairs = [(i, (i + by) % count) for i in range(count) if closed or i + by in range(count)]
    return lax.ppermute(block, axis, pairs)


def fold_exchange(own, from_west, from_east, seam, width, beside):
    around, height = lax.axis_size(GX), lax.axis_size("gy")
    centre = (seam[0] // width + lax.axis_index(GX)) % around
    part = (centre + 1) % 3
    held = jnp.where(part == 0, from_west, jnp.where(part == 2, from_east, own))

    def mirror(coarse):
        pairs = [
            (i * height + height - 1, (3 * coarse - i) % around * height + height - 1) for i in range(around)
        ]

        def branch(rows, arrays):
            return lax.ppermute(rows, GX + ("gy",), pairs), beside(*arrays)

        return branch

    return (centre + 1) // 3, [mirror(coarse) for coarse in range((around + 2) // 3)], held


def shards(heat, brine, currents, sea, layers, area, rain, seam):
    _, _, width = heat.shape
    sums = local_sums(brine, sea, area, rain, lax.axis_size(NEAR))
    plane = all_sum(sums, NEAR)
    west_own, east_own, south_own, north_own, fold_own = packs(heat, brine, currents, sea, layers)
    plane, west_own, east_own, south_own, north_own = lax.optimization_barrier(
        (plane, west_own, east_own, south_own, north_own)
    )
    totals = all_sum(jnp.broadcast_to(plane[None], (lax.axis_size("chip"),) + plane.shape), "chip")
    west_halo = along(east_own, GX, 1, True)
    east_halo = along(west_own, GX, -1, True)
    south_halo = along(north_own, "gy", 1, False)
    north_halo = along(south_own, "gy", -1, False)
    place, branches, held = fold_exchange(fold_own, west_halo[32:], east_halo[24:], seam, width, tracer_step)
    arrays = (
        heat, brine, currents, sea, layers, area,
        west_own, east_own, west_halo, east_halo, south_halo, north_halo,
    )
    fold_halo, (heat_next, salt_next) = lax.switch(place, branches, held, arrays)
    heat_next, salt_next = close_fold(heat_next, salt_next, north_own, fold_halo, area)
    return heat_next, add_virtual(salt_next, brine, rain, sea, totals)


def solution(mesh):
    chips = mesh.shape["gx"] // CORES
    split = Mesh(
        mesh.devices.reshape(mesh.shape["groups"], chips, CORES, mesh.shape["gy"]), ("groups",) + GX + ("gy",)
    )
    cells = P("groups", "gy", GX)
    plane = P("gy", GX)
    in_specs = (cells, cells, P("groups", None, "gy", GX), plane, plane, plane, plane, P(GX))
    return jax.shard_map(
        shards, mesh=split, in_specs=in_specs, out_specs=(cells, cells), check_vma=False
    )
```

```python
import jax
import jax.numpy as jnp
from jax import lax
from jax.experimental import pallas as pl
from jax.experimental.pallas import tpu as pltpu
from jax.sharding import Mesh
from jax.sharding import PartitionSpec as P


time_step = 0.25
diffusivity = 0.5
vertical_mixing = 0.3
top_thickness = 0.5

VMEM = pl.BlockSpec(memory_space=pltpu.VMEM)
LANES = 128
CORES = 2
GX = ("chip", "core")
NEAR = ("core", "gy")


def lane_of(shape):
    return lax.broadcasted_iota(jnp.int32, shape, len(shape) - 1)


def sums_kernel(surface, sea, area, rain, out):
    wet_area = area[...] * sea[...].astype(jnp.float32)
    salt = wet_area * surface[0]
    rain_now = rain[...]
    lane = lane_of((1, LANES))
    packed = jnp.zeros((1, LANES), jnp.float32)
    for place, field in enumerate((wet_area, wet_area * rain_now, salt * rain_now, salt)):
        total = jnp.sum(jnp.sum(field, axis=0, keepdims=True), axis=1, keepdims=True)
        packed = jnp.where(lane == place, total, packed)
    out[...] = jnp.broadcast_to(packed[None], out.shape)


def local_sums(brine, sea, area, rain, copies):
    rows, width = sea.shape
    plane = pl.BlockSpec((rows, width), lambda i: (0, 0))
    return pl.pallas_call(
        sums_kernel,
        grid=(1,),
        in_specs=[pl.BlockSpec((1, rows, width), lambda i: (0, 0, 0)), plane, plane, plane],
        out_specs=pl.BlockSpec((copies, 1, LANES), lambda i: (0, 0, 0)),
        out_shape=jax.ShapeDtypeStruct((copies, 1, LANES), jnp.float32),
        name="local_sums",
    )(brine, sea, area, rain)


def mirrored(rows):
    lane = lane_of(rows.shape)
    bit = 1
    while bit < LANES:
        low = (lane // bit) % 2 == 0
        rows = jnp.where(low, pltpu.roll(rows, LANES - bit, 1), pltpu.roll(rows, bit, 1))
        bit *= 2
    return rows


def column_pack(planes, lane_number):
    lane = lane_of((8, LANES))
    blocks = planes[0].shape[0] // 8
    packed = jnp.zeros((8, LANES), jnp.float32)
    for level, plane in enumerate(planes):
        for block in range(blocks):
            place = level * blocks + block
            tile = plane[8 * block : 8 * block + 8]
            moved = pltpu.roll(tile, (place - lane_number) % LANES, 1)
            packed = jnp.where(lane == place, moved, packed)
    return packed


def pack_kernel(heat, salt, currents, sea, layers, west, east, south, north, fold):
    levels, rows, _ = heat.shape
    depth = (sea[...] * layers[...]).astype(jnp.float32)
    heat_planes = [heat[k] for k in range(levels)]
    salt_planes = [salt[k] for k in range(levels)]
    speed_planes = [currents[0, k] for k in range(levels)]
    depth_planes = [depth] * levels
    west[0:8] = column_pack(heat_planes, 0)
    west[8:16] = column_pack(salt_planes, 0)
    west[16:24] = column_pack(depth_planes, 0)
    east[0:8] = column_pack(heat_planes, LANES - 1)
    east[8:16] = column_pack(salt_planes, LANES - 1)
    east[16:24] = column_pack(depth_planes, LANES - 1)
    east[24:32] = column_pack(speed_planes, LANES - 1)
    last = rows - 1
    for k in range(levels):
        south[k : k + 1] = heat[k, 0:1]
        south[levels + k : levels + k + 1] = salt[k, 0:1]
        north[k : k + 1] = heat[k, last:rows]
        north[levels + k : levels + k + 1] = salt[k, last:rows]
        north[2 * levels + 8 + k : 2 * levels + 9 + k] = currents[1, k, last:rows]
    south[2 * levels : 2 * levels + 8] = jnp.broadcast_to(depth[0:1], (8, LANES))
    north[2 * levels : 2 * levels + 8] = jnp.broadcast_to(depth[last:rows], (8, LANES))
    turned = mirrored(north[...])
    fold[...] = turned
    west[24:] = turned
    east[32:] = turned


def packs(heat, salt, currents, sea, layers):
    levels, _, _ = heat.shape
    north = 3 * levels + 8
    shapes = (24 + north, 32 + north, 2 * levels + 8, north, north)
    return pl.pallas_call(
        pack_kernel,
        in_specs=[VMEM] * 5,
        out_specs=[VMEM] * 5,
        out_shape=[jax.ShapeDtypeStruct((n, LANES), jnp.float32) for n in shapes],
        name="edge_packs",
    )(heat, salt, currents, sea, layers)


def open_flux(near, far, forward, backward):
    return forward * near + backward * far - diffusivity * (far - near)


def edge_flux(near, far, speed, near_depth, far_depth, level):
    wet = (level < jnp.minimum(near_depth, far_depth)).astype(jnp.float32)
    return wet * open_flux(near, far, jnp.maximum(speed, 0.0), jnp.minimum(speed, 0.0))


def step_kernel(
    heat, salt, currents, sea, layers, area,
    west_own, east_own, west_halo, east_halo,
    heat_out, salt_out,
):
    levels, rows, _ = heat.shape
    blocks = rows // 8
    lane = lane_of((rows, LANES))
    row = lax.broadcasted_iota(jnp.int32, (rows, LANES), 0)
    first_lane, last_lane = lane == 0, lane == LANES - 1
    last_row = row == rows - 1
    depth = (sea[...] * layers[...]).astype(jnp.float32)
    open_north = jnp.where(last_row, 0.0, jnp.minimum(depth, pltpu.roll(depth, rows - 1, 0)))
    open_east = jnp.where(last_lane, 0.0, jnp.minimum(depth, pltpu.roll(depth, LANES - 1, 1)))
    per_area = time_step / area[...]
    edge_level = (lane_of((8, LANES)) // blocks).astype(jnp.float32)
    west_edge, east_edge = [], []
    for f in range(2):
        own_west, own_east = west_own[8 * f : 8 * f + 8], east_own[8 * f : 8 * f + 8]
        west_edge.append(
            edge_flux(west_halo[8 * f : 8 * f + 8], own_west, west_halo[24:32], west_halo[16:24], west_own[16:24], edge_level)
        )
        east_edge.append(
            edge_flux(own_east, east_halo[8 * f : 8 * f + 8], east_own[24:32], east_own[16:24], east_halo[16:24], edge_level)
        )
    fields = (heat, salt)

    def one_level(k, above):
        level = k.astype(jnp.float32)
        east_speed, north_speed = currents[0, k], currents[1, k]
        east_up, east_down = jnp.maximum(east_speed, 0.0), jnp.minimum(east_speed, 0.0)
        north_up, north_down = jnp.maximum(north_speed, 0.0), jnp.minimum(north_speed, 0.0)
        east_wet = level < open_east
        north_wet = level < open_north
        wet = level < depth
        below_wet = level + 1.0 < depth
        passed = []
        for f in range(2):
            cells = fields[f][k]
            east_flux = jnp.where(
                east_wet, open_flux(cells, pltpu.roll(cells, LANES - 1, 1), east_up, east_down), 0.0
            )
            west_flux = pltpu.roll(east_flux, 1, 1)
            west_columns, east_columns = [], []
            for block in range(blocks):
                place = k * blocks + block
                west_columns.append(pltpu.roll(west_edge[f], (LANES - place) % LANES, 1))
                east_columns.append(pltpu.roll(east_edge[f], LANES - 1 - place, 1))
            west_flux = jnp.where(first_lane, jnp.concatenate(west_columns, axis=0), west_flux)
            east_flux = jnp.where(last_lane, jnp.concatenate(east_columns, axis=0), east_flux)
            northern = pltpu.roll(cells, rows - 1, 0)
            north_flux = jnp.where(north_wet, open_flux(cells, northern, north_up, north_down), 0.0)
            south_flux = pltpu.roll(north_flux, 1, 0)
            next_cells = fields[f][jnp.minimum(k + 1, levels - 1)]
            below = jnp.where(below_wet, vertical_mixing * (cells - next_cells), 0.0)
            change = per_area * (west_flux - east_flux + south_flux - north_flux) + time_step * (above[f] - below)
            (heat_out, salt_out)[f][k] = cells + jnp.where(wet, change, 0.0)
            passed.append(below)
        return tuple(passed)

    nothing = jnp.zeros((rows, LANES), jnp.float32)
    lax.fori_loop(0, levels, one_level, (nothing, nothing))


def tracer_step(*arrays):
    heat = arrays[0]
    return pl.pallas_call(
        step_kernel,
        in_specs=[VMEM] * 10,
        out_specs=[VMEM] * 2,
        out_shape=[jax.ShapeDtypeStruct(heat.shape, jnp.float32)] * 2,
        name="tracer_step",
    )(*arrays)


def edge_kernel(
    flags, heat_next, salt_next, south_own, north_own, south_halo, north_halo, fold_halo, area, heat_out, salt_out
):
    levels, band, _ = heat_next.shape
    base = 2 * levels
    level = lax.broadcasted_iota(jnp.int32, (levels, LANES), 0).astype(jnp.float32)
    row = lax.broadcasted_iota(jnp.int32, (band, LANES), 0)
    is_top = flags[0] == 1
    fields = ((heat_next, heat_out), (salt_next, salt_out))

    def cells(rows, f):
        return rows[f * levels : f * levels + levels]

    @pl.when(pl.program_id(0) == 0)
    def _():
        for f, (before, after) in enumerate(fields):
            flux = edge_flux(
                cells(south_halo, f), cells(south_own, f), south_halo[base + 8 :],
                south_halo[base : base + 1], south_own[base : base + 1], level,
            )
            entering = time_step / area[0:1] * flux
            for k in range(levels):
                after[k] = before[k] + jnp.where(row == 0, entering[k : k + 1], 0.0)

    @pl.when(pl.program_id(0) == 1)
    def _():
        speed = north_own[base + 8 :]
        speed = jnp.where(is_top, 0.5 * (speed - fold_halo[base + 8 :]), speed)
        far_depth = jnp.where(is_top, fold_halo[base : base + 1], north_halo[base : base + 1])
        for f, (before, after) in enumerate(fields):
            far = jnp.where(is_top, cells(fold_halo, f), cells(north_halo, f))
            flux = edge_flux(cells(north_own, f), far, speed, north_own[base : base + 1], far_depth, level)
            leaving = time_step / area[band - 1 : band] * flux
            for k in range(levels):
                after[k] = before[k] - jnp.where(row == band - 1, leaving[k : k + 1], 0.0)


def close_edges(is_top, heat_next, salt_next, south_own, north_own, south_halo, north_halo, fold_halo, area):
    levels, rows, width = heat_next.shape
    gap = rows // 8 - 1
    band = pl.BlockSpec((levels, 8, width), lambda i: (0, i * gap, 0))

    def whole(rows):
        return pl.BlockSpec(rows.shape, lambda i: (0, 0))

    packs = (south_own, north_own, south_halo, north_halo, fold_halo)
    return pl.pallas_call(
        edge_kernel,
        grid=(2,),
        in_specs=[pl.BlockSpec(memory_space=pltpu.SMEM), band, band]
        + [whole(rows) for rows in packs]
        + [pl.BlockSpec((8, width), lambda i: (i * gap, 0))],
        out_specs=[band, band],
        out_shape=[jax.ShapeDtypeStruct(heat_next.shape, jnp.float32)] * 2,
        input_output_aliases={1: 0, 2: 1},
        name="close_edges",
    )(is_top, heat_next, salt_next, *packs, area)


def final_kernel(salt_next, surface, rain, sea, totals, out):
    lane = lane_of((1, LANES))
    summed = jnp.sum(totals[...], axis=0)

    def total(place):
        return jnp.sum(jnp.where(lane == place, summed, 0.0), axis=1, keepdims=True)

    total_area, total_fresh, salt_fresh, salt_only = (total(place) for place in range(4))
    mean_fresh = total_fresh / total_area
    total_salt = salt_fresh - mean_fresh * salt_only
    balanced = rain[...] - mean_fresh
    virtual = -surface[0] * balanced + total_salt / total_area
    wet = (sea[...] > 0).astype(jnp.float32)
    out[0] = salt_next[0] + time_step / top_thickness * virtual * wet


def add_virtual(salt_next, brine, rain, sea, totals):
    _, rows, width = salt_next.shape
    plane = pl.BlockSpec((rows, width), lambda i: (0, 0))
    top = pl.BlockSpec((1, rows, width), lambda i: (0, 0, 0))
    return pl.pallas_call(
        final_kernel,
        grid=(1,),
        in_specs=[top, top, plane, plane, pl.BlockSpec(totals.shape, lambda i: (0, 0, 0))],
        out_specs=top,
        out_shape=jax.ShapeDtypeStruct(salt_next.shape, jnp.float32),
        input_output_aliases={0: 0},
        name="add_virtual",
    )(salt_next, brine, rain, sea, totals)


def share(copies, axes):
    return lax.all_to_all(copies, axes, 0, 0, tiled=True)


def along(block, axis, by, closed):
    count = lax.axis_size(axis)
    pairs = [(i, (i + by) % count) for i in range(count) if closed or i + by in range(count)]
    return lax.ppermute(block, axis, pairs)


def fold_exchange(own, from_west, from_east, seam, width, beside):
    around, height = lax.axis_size(GX), lax.axis_size("gy")
    centre = (seam[0] // width + lax.axis_index(GX)) % around
    part = (centre + 1) % 3
    held = jnp.where(part == 0, from_west, jnp.where(part == 2, from_east, own))

    def mirror(coarse):
        pairs = [
            (i * height + height - 1, (3 * coarse - i) % around * height + height - 1) for i in range(around)
        ]

        def branch(rows, arrays):
            return lax.ppermute(rows, GX + ("gy",), pairs), beside(*arrays)

        return branch

    return (centre + 1) // 3, [mirror(coarse) for coarse in range((around + 2) // 3)], held


def shards(heat, brine, currents, sea, layers, area, rain, seam):
    _, _, width = heat.shape
    sums = local_sums(brine, sea, area, rain, lax.axis_size(NEAR))
    plane = jnp.sum(share(sums, NEAR), axis=0)
    totals = share(jnp.broadcast_to(plane[None], (lax.axis_size("chip"),) + plane.shape), "chip")
    west_own, east_own, south_own, north_own, fold_own = packs(heat, brine, currents, sea, layers)
    west_halo = along(east_own, GX, 1, True)
    east_halo = along(west_own, GX, -1, True)
    place, branches, held = fold_exchange(fold_own, west_halo[32:], east_halo[24:], seam, width, tracer_step)
    arrays = (heat, brine, currents, sea, layers, area, west_own, east_own, west_halo, east_halo)
    fold_halo, (heat_next, salt_next) = lax.switch(place, branches, held, arrays)
    north_sent, south_sent, fold_halo = lax.optimization_barrier((north_own, south_own, fold_halo))
    south_halo = along(north_sent, "gy", 1, False)
    north_halo = along(south_sent, "gy", -1, False)
    is_top = (lax.axis_index("gy") == lax.axis_size("gy") - 1).astype(jnp.int32)
    heat_next, salt_next = close_edges(
        is_top[None], heat_next, salt_next, south_own, north_own, south_halo, north_halo, fold_halo, area
    )
    return heat_next, add_virtual(salt_next, brine, rain, sea, totals)


def solution(mesh):
    chips = mesh.shape["gx"] // CORES
    split = Mesh(
        mesh.devices.reshape(mesh.shape["groups"], chips, CORES, mesh.shape["gy"]), ("groups",) + GX + ("gy",)
    )
    cells = P("groups", "gy", GX)
    plane = P("gy", GX)
    in_specs = (cells, cells, P("groups", None, "gy", GX), plane, plane, plane, plane, P(GX))
    return jax.shard_map(
        shards, mesh=split, in_specs=in_specs, out_specs=(cells, cells), check_vma=False
    )
```

```python
import jax
import jax.numpy as jnp
from jax import lax
from jax.experimental import pallas as pl
from jax.experimental.pallas import tpu as pltpu
from jax.sharding import Mesh
from jax.sharding import PartitionSpec as P


time_step = 0.25
diffusivity = 0.5
vertical_mixing = 0.3
top_thickness = 0.5

VMEM = pl.BlockSpec(memory_space=pltpu.VMEM)
LANES = 128
CORES = 2
GX = ("chip", "core")
NEAR = ("core", "gy")


def lane_of(shape):
    return lax.broadcasted_iota(jnp.int32, shape, len(shape) - 1)


def sums_kernel(surface, sea, area, rain, out):
    wet_area = area[...] * sea[...].astype(jnp.float32)
    salt = wet_area * surface[0]
    rain_now = rain[...]
    lane = lane_of((1, LANES))
    packed = jnp.zeros((1, LANES), jnp.float32)
    for place, field in enumerate((wet_area, wet_area * rain_now, salt * rain_now, salt)):
        total = jnp.sum(jnp.sum(field, axis=0, keepdims=True), axis=1, keepdims=True)
        packed = jnp.where(lane == place, total, packed)
    out[...] = jnp.broadcast_to(packed[None], out.shape)


def local_sums(brine, sea, area, rain, copies):
    rows, width = sea.shape
    plane = pl.BlockSpec((rows, width), lambda i: (0, 0))
    return pl.pallas_call(
        sums_kernel,
        grid=(1,),
        in_specs=[pl.BlockSpec((1, rows, width), lambda i: (0, 0, 0)), plane, plane, plane],
        out_specs=pl.BlockSpec((copies, 1, LANES), lambda i: (0, 0, 0)),
        out_shape=jax.ShapeDtypeStruct((copies, 1, LANES), jnp.float32),
        name="local_sums",
    )(brine, sea, area, rain)


def mirrored(rows):
    lane = lane_of(rows.shape)
    bit = 1
    while bit < LANES:
        low = (lane // bit) % 2 == 0
        rows = jnp.where(low, pltpu.roll(rows, LANES - bit, 1), pltpu.roll(rows, bit, 1))
        bit *= 2
    return rows


def column_pack(planes, lane_number):
    lane = lane_of((8, LANES))
    blocks = planes[0].shape[0] // 8
    packed = jnp.zeros((8, LANES), jnp.float32)
    for level, plane in enumerate(planes):
        for block in range(blocks):
            place = level * blocks + block
            tile = plane[8 * block : 8 * block + 8]
            moved = pltpu.roll(tile, (place - lane_number) % LANES, 1)
            packed = jnp.where(lane == place, moved, packed)
    return packed


def pack_kernel(heat, salt, currents, sea, layers, west, east, south, north, fold):
    levels, rows, _ = heat.shape
    depth = (sea[...] * layers[...]).astype(jnp.float32)
    heat_planes = [heat[k] for k in range(levels)]
    salt_planes = [salt[k] for k in range(levels)]
    speed_planes = [currents[0, k] for k in range(levels)]
    depth_planes = [depth] * levels
    west[0:8] = column_pack(heat_planes, 0)
    west[8:16] = column_pack(salt_planes, 0)
    west[16:24] = column_pack(depth_planes, 0)
    east[0:8] = column_pack(heat_planes, LANES - 1)
    east[8:16] = column_pack(salt_planes, LANES - 1)
    east[16:24] = column_pack(depth_planes, LANES - 1)
    east[24:32] = column_pack(speed_planes, LANES - 1)
    last = rows - 1
    for k in range(levels):
        south[k : k + 1] = heat[k, 0:1]
        south[levels + k : levels + k + 1] = salt[k, 0:1]
        north[k : k + 1] = heat[k, last:rows]
        north[levels + k : levels + k + 1] = salt[k, last:rows]
        north[2 * levels + 8 + k : 2 * levels + 9 + k] = currents[1, k, last:rows]
    south[2 * levels : 2 * levels + 8] = jnp.broadcast_to(depth[0:1], (8, LANES))
    north[2 * levels : 2 * levels + 8] = jnp.broadcast_to(depth[last:rows], (8, LANES))
    turned = mirrored(north[...])
    fold[...] = turned
    west[24:] = turned
    east[32:] = turned


def packs(heat, salt, currents, sea, layers):
    levels, _, _ = heat.shape
    north = 3 * levels + 8
    shapes = (24 + north, 32 + north, 2 * levels + 8, north, north)
    return pl.pallas_call(
        pack_kernel,
        in_specs=[VMEM] * 5,
        out_specs=[VMEM] * 5,
        out_shape=[jax.ShapeDtypeStruct((n, LANES), jnp.float32) for n in shapes],
        name="edge_packs",
    )(heat, salt, currents, sea, layers)


def open_flux(near, far, forward, backward):
    return forward * near + backward * far - diffusivity * (far - near)


def edge_flux(near, far, speed, near_depth, far_depth, level):
    wet = (level < jnp.minimum(near_depth, far_depth)).astype(jnp.float32)
    return wet * open_flux(near, far, jnp.maximum(speed, 0.0), jnp.minimum(speed, 0.0))


def step_kernel(
    heat, salt, currents, sea, layers, area,
    west_own, east_own, west_halo, east_halo, south_halo, north_halo,
    heat_out, salt_out,
):
    levels, rows, _ = heat.shape
    blocks = rows // 8
    lane = lane_of((rows, LANES))
    row = lax.broadcasted_iota(jnp.int32, (rows, LANES), 0)
    first_lane, last_lane = lane == 0, lane == LANES - 1
    first_row, last_row = row == 0, row == rows - 1
    depth = (sea[...] * layers[...]).astype(jnp.float32)
    base = 2 * levels
    south_depth = south_halo[base : base + 1]
    depth_north = jnp.where(last_row, north_halo[base : base + 1], pltpu.roll(depth, rows - 1, 0))
    open_north = jnp.minimum(depth, depth_north)
    open_south = jnp.minimum(depth[0:1], south_depth)
    open_east = jnp.where(last_lane, 0.0, jnp.minimum(depth, pltpu.roll(depth, LANES - 1, 1)))
    per_area = time_step / area[...]
    edge_level = (lane_of((8, LANES)) // blocks).astype(jnp.float32)
    west_edge, east_edge = [], []
    for f in range(2):
        own_west, own_east = west_own[8 * f : 8 * f + 8], east_own[8 * f : 8 * f + 8]
        west_edge.append(
            edge_flux(west_halo[8 * f : 8 * f + 8], own_west, west_halo[24:32], west_halo[16:24], west_own[16:24], edge_level)
        )
        east_edge.append(
            edge_flux(own_east, east_halo[8 * f : 8 * f + 8], east_own[24:32], east_own[16:24], east_halo[16:24], edge_level)
        )
    fields = (heat, salt)

    def one_level(k, above):
        level = k.astype(jnp.float32)
        east_speed, north_speed = currents[0, k], currents[1, k]
        south_speed = south_halo[pl.ds(base + 8 + k, 1)]
        east_up, east_down = jnp.maximum(east_speed, 0.0), jnp.minimum(east_speed, 0.0)
        north_up, north_down = jnp.maximum(north_speed, 0.0), jnp.minimum(north_speed, 0.0)
        east_wet = level < open_east
        north_wet = level < open_north
        wet = level < depth
        below_wet = level + 1.0 < depth
        passed = []
        for f in range(2):
            cells = fields[f][k]
            at = f * levels + k
            east_flux = jnp.where(
                east_wet, open_flux(cells, pltpu.roll(cells, LANES - 1, 1), east_up, east_down), 0.0
            )
            west_flux = pltpu.roll(east_flux, 1, 1)
            west_columns, east_columns = [], []
            for block in range(blocks):
                place = k * blocks + block
                west_columns.append(pltpu.roll(west_edge[f], (LANES - place) % LANES, 1))
                east_columns.append(pltpu.roll(east_edge[f], LANES - 1 - place, 1))
            west_flux = jnp.where(first_lane, jnp.concatenate(west_columns, axis=0), west_flux)
            east_flux = jnp.where(last_lane, jnp.concatenate(east_columns, axis=0), east_flux)
            northern = jnp.where(last_row, north_halo[pl.ds(at, 1)], pltpu.roll(cells, rows - 1, 0))
            north_flux = jnp.where(north_wet, open_flux(cells, northern, north_up, north_down), 0.0)
            first_flux = edge_flux(
                south_halo[pl.ds(at, 1)], cells[0:1], south_speed, open_south, open_south, level
            )
            south_flux = jnp.where(first_row, first_flux, pltpu.roll(north_flux, 1, 0))
            next_cells = fields[f][jnp.minimum(k + 1, levels - 1)]
            below = jnp.where(below_wet, vertical_mixing * (cells - next_cells), 0.0)
            change = per_area * (west_flux - east_flux + south_flux - north_flux) + time_step * (above[f] - below)
            (heat_out, salt_out)[f][k] = cells + jnp.where(wet, change, 0.0)
            passed.append(below)
        return tuple(passed)

    nothing = jnp.zeros((rows, LANES), jnp.float32)
    lax.fori_loop(0, levels, one_level, (nothing, nothing))


def tracer_step(*arrays):
    heat = arrays[0]
    return pl.pallas_call(
        step_kernel,
        in_specs=[VMEM] * 12,
        out_specs=[VMEM] * 2,
        out_shape=[jax.ShapeDtypeStruct(heat.shape, jnp.float32)] * 2,
        name="tracer_step",
    )(*arrays)


def fold_kernel(heat_next, salt_next, own, fold, area, heat_out, salt_out):
    levels, band, _ = heat_next.shape
    base = 2 * levels
    level = lax.broadcasted_iota(jnp.int32, (levels, LANES), 0).astype(jnp.float32)
    per_area = time_step / area[band - 1 : band]
    speed = 0.5 * (own[base + 8 :] - fold[base + 8 :])
    last = lax.broadcasted_iota(jnp.int32, (band, LANES), 0) == band - 1
    for f, (before, after) in enumerate(((heat_next, heat_out), (salt_next, salt_out))):
        flux = edge_flux(
            own[f * levels : f * levels + levels], fold[f * levels : f * levels + levels], speed,
            own[base : base + 1], fold[base : base + 1], level,
        )
        leaving = per_area * flux
        for k in range(levels):
            after[k] = before[k] - jnp.where(last, leaving[k : k + 1], 0.0)


def close_fold(heat_next, salt_next, own, fold, area):
    levels, rows, width = heat_next.shape
    band = pl.BlockSpec((levels, 8, width), lambda i: (0, rows // 8 - 1, 0))
    whole = pl.BlockSpec(own.shape, lambda i: (0, 0))
    return pl.pallas_call(
        fold_kernel,
        grid=(1,),
        in_specs=[band, band, whole, whole, pl.BlockSpec((8, width), lambda i: (rows // 8 - 1, 0))],
        out_specs=[band, band],
        out_shape=[jax.ShapeDtypeStruct(heat_next.shape, jnp.float32)] * 2,
        input_output_aliases={0: 0, 1: 1},
        name="close_fold",
    )(heat_next, salt_next, own, fold, area)


def final_kernel(salt_next, surface, rain, sea, totals, out):
    lane = lane_of((1, LANES))

    def total(place):
        return jnp.sum(jnp.where(lane == place, totals[...], 0.0), axis=1, keepdims=True)

    total_area, total_fresh, salt_fresh, salt_only = (total(place) for place in range(4))
    mean_fresh = total_fresh / total_area
    total_salt = salt_fresh - mean_fresh * salt_only
    balanced = rain[...] - mean_fresh
    virtual = -surface[0] * balanced + total_salt / total_area
    wet = (sea[...] > 0).astype(jnp.float32)
    out[0] = salt_next[0] + time_step / top_thickness * virtual * wet


def add_virtual(salt_next, brine, rain, sea, totals):
    _, rows, width = salt_next.shape
    plane = pl.BlockSpec((rows, width), lambda i: (0, 0))
    top = pl.BlockSpec((1, rows, width), lambda i: (0, 0, 0))
    return pl.pallas_call(
        final_kernel,
        grid=(1,),
        in_specs=[top, top, plane, plane, pl.BlockSpec((1, LANES), lambda i: (0, 0))],
        out_specs=top,
        out_shape=jax.ShapeDtypeStruct(salt_next.shape, jnp.float32),
        input_output_aliases={0: 0},
        name="add_virtual",
    )(salt_next, brine, rain, sea, totals)


def share(copies, axes):
    return lax.all_to_all(copies, axes, 0, 0, tiled=True)


def along(block, axis, by, closed):
    count = lax.axis_size(axis)
    pairs = [(i, (i + by) % count) for i in range(count) if closed or i + by in range(count)]
    return lax.ppermute(block, axis, pairs)


def fold_branches(beside):
    around, height = lax.axis_size(GX), lax.axis_size("gy")

    def mirror(coarse):
        pairs = [
            (i * height + height - 1, (3 * coarse - i) % around * height + height - 1) for i in range(around)
        ]

        def branch(rows, arrays, south_own, north_own):
            fold_halo = lax.ppermute(rows, GX + ("gy",), pairs)
            south_halo = along(north_own, "gy", 1, False)
            north_halo = along(south_own, "gy", -1, False)
            return fold_halo, beside(*arrays, south_halo, north_halo)

        return branch

    return [mirror(coarse) for coarse in range((around + 2) // 3)]


def shards(heat, brine, currents, sea, layers, area, rain, seam):
    _, _, width = heat.shape
    sums = local_sums(brine, sea, area, rain, lax.axis_size(NEAR))
    plane = jnp.sum(share(sums, NEAR), axis=0)
    centre = (seam[0] // width + lax.axis_index(GX)) % lax.axis_size(GX)
    place, part = (centre + 1) // 3, (centre + 1) % 3
    layers, place, part = lax.optimization_barrier((layers, place, part))
    west_own, east_own, south_own, north_own, fold_own = packs(heat, brine, currents, sea, layers)
    totals = share(jnp.broadcast_to(plane[None], (lax.axis_size("chip"),) + plane.shape), "chip")
    totals = jnp.sum(totals, axis=0)
    west_halo = along(east_own, GX, 1, True)
    east_halo = along(west_own, GX, -1, True)
    held = jnp.where(part == 0, west_halo[32:], jnp.where(part == 2, east_halo[24:], fold_own))
    arrays = (heat, brine, currents, sea, layers, area, west_own, east_own, west_halo, east_halo)
    fold_halo, (heat_next, salt_next) = lax.switch(
        place, fold_branches(tracer_step), held, arrays, south_own, north_own
    )
    heat_next, salt_next = close_fold(heat_next, salt_next, north_own, fold_halo, area)
    return heat_next, add_virtual(salt_next, brine, rain, sea, totals)


def solution(mesh):
    chips = mesh.shape["gx"] // CORES
    split = Mesh(
        mesh.devices.reshape(mesh.shape["groups"], chips, CORES, mesh.shape["gy"]), ("groups",) + GX + ("gy",)
    )
    cells = P("groups", "gy", GX)
    plane = P("gy", GX)
    in_specs = (cells, cells, P("groups", None, "gy", GX), plane, plane, plane, plane, P(GX))
    return jax.shard_map(
        shards, mesh=split, in_specs=in_specs, out_specs=(cells, cells), check_vma=False
    )
```

```python
import jax
import jax.numpy as jnp
from jax import lax
from jax.experimental import pallas as pl
from jax.experimental.pallas import tpu as pltpu
from jax.sharding import Mesh
from jax.sharding import PartitionSpec as P


time_step = 0.25
diffusivity = 0.5
vertical_mixing = 0.3
top_thickness = 0.5

VMEM = pl.BlockSpec(memory_space=pltpu.VMEM)
LANES = 128
CORES = 2
GX = ("chip", "core")
NEAR = ("core", "gy")


def lane_of(shape):
    return lax.broadcasted_iota(jnp.int32, shape, len(shape) - 1)


def sums_kernel(surface, sea, area, rain, out):
    wet_area = area[...] * sea[...].astype(jnp.float32)
    salt = wet_area * surface[0]
    rain_now = rain[...]
    lane = lane_of((1, LANES))
    packed = jnp.zeros((1, LANES), jnp.float32)
    for place, field in enumerate((wet_area, wet_area * rain_now, salt * rain_now, salt)):
        total = jnp.sum(jnp.sum(field, axis=0, keepdims=True), axis=1, keepdims=True)
        packed = jnp.where(lane == place, total, packed)
    out[...] = jnp.broadcast_to(packed[None], out.shape)


def local_sums(brine, sea, area, rain, copies):
    rows, width = sea.shape
    plane = pl.BlockSpec((rows, width), lambda i: (0, 0))
    return pl.pallas_call(
        sums_kernel,
        grid=(1,),
        in_specs=[pl.BlockSpec((1, rows, width), lambda i: (0, 0, 0)), plane, plane, plane],
        out_specs=pl.BlockSpec((copies, 1, LANES), lambda i: (0, 0, 0)),
        out_shape=jax.ShapeDtypeStruct((copies, 1, LANES), jnp.float32),
        name="local_sums",
    )(brine, sea, area, rain)


def mirrored(rows):
    lane = lane_of(rows.shape)
    bit = 1
    while bit < LANES:
        low = (lane // bit) % 2 == 0
        rows = jnp.where(low, pltpu.roll(rows, LANES - bit, 1), pltpu.roll(rows, bit, 1))
        bit *= 2
    return rows


def column_pack(planes, lane_number):
    lane = lane_of((8, LANES))
    blocks = planes[0].shape[0] // 8
    packed = jnp.zeros((8, LANES), jnp.float32)
    for level, plane in enumerate(planes):
        for block in range(blocks):
            place = level * blocks + block
            tile = plane[8 * block : 8 * block + 8]
            moved = pltpu.roll(tile, (place - lane_number) % LANES, 1)
            packed = jnp.where(lane == place, moved, packed)
    return packed


def pack_kernel(heat, salt, currents, sea, layers, west, east, south, north, fold):
    levels, rows, _ = heat.shape
    depth = (sea[...] * layers[...]).astype(jnp.float32)
    heat_planes = [heat[k] for k in range(levels)]
    salt_planes = [salt[k] for k in range(levels)]
    speed_planes = [currents[0, k] for k in range(levels)]
    depth_planes = [depth] * levels
    west[0:8] = column_pack(heat_planes, 0)
    west[8:16] = column_pack(salt_planes, 0)
    west[16:24] = column_pack(depth_planes, 0)
    east[0:8] = column_pack(heat_planes, LANES - 1)
    east[8:16] = column_pack(salt_planes, LANES - 1)
    east[16:24] = column_pack(depth_planes, LANES - 1)
    east[24:32] = column_pack(speed_planes, LANES - 1)
    last = rows - 1
    for k in range(levels):
        south[k : k + 1] = heat[k, 0:1]
        south[levels + k : levels + k + 1] = salt[k, 0:1]
        north[k : k + 1] = heat[k, last:rows]
        north[levels + k : levels + k + 1] = salt[k, last:rows]
        north[2 * levels + 8 + k : 2 * levels + 9 + k] = currents[1, k, last:rows]
    south[2 * levels : 2 * levels + 8] = jnp.broadcast_to(depth[0:1], (8, LANES))
    north[2 * levels : 2 * levels + 8] = jnp.broadcast_to(depth[last:rows], (8, LANES))
    level = lax.broadcasted_iota(jnp.int32, (levels, LANES), 0).astype(jnp.float32)
    fold[0:levels] = mirrored(north[0:levels])
    fold[levels : 2 * levels] = mirrored(
        jnp.where(level < depth[last:rows], north[levels : 2 * levels], 0.0)
    )
    fold[2 * levels :] = mirrored(north[2 * levels + 8 :])
    west[24:] = fold[...]
    east[32:] = fold[...]


def packs(heat, salt, currents, sea, layers):
    levels, _, _ = heat.shape
    north = 3 * levels + 8
    shapes = (24 + 3 * levels, 32 + 3 * levels, 2 * levels + 8, north, 3 * levels)
    return pl.pallas_call(
        pack_kernel,
        in_specs=[VMEM] * 5,
        out_specs=[VMEM] * 5,
        out_shape=[jax.ShapeDtypeStruct((n, LANES), jnp.float32) for n in shapes],
        name="edge_packs",
    )(heat, salt, currents, sea, layers)


def open_flux(near, far, forward, backward):
    return forward * near + backward * far - diffusivity * (far - near)


def edge_flux(near, far, speed, near_depth, far_depth, level):
    wet = (level < jnp.minimum(near_depth, far_depth)).astype(jnp.float32)
    return wet * open_flux(near, far, jnp.maximum(speed, 0.0), jnp.minimum(speed, 0.0))


def step_kernel(
    heat, salt, currents, sea, layers, area,
    west_own, east_own, west_halo, east_halo, south_halo, north_halo,
    heat_out, salt_out,
):
    levels, rows, _ = heat.shape
    blocks = rows // 8
    lane = lane_of((rows, LANES))
    row = lax.broadcasted_iota(jnp.int32, (rows, LANES), 0)
    first_lane, last_lane = lane == 0, lane == LANES - 1
    first_row, last_row = row == 0, row == rows - 1
    depth = (sea[...] * layers[...]).astype(jnp.float32)
    base = 2 * levels
    south_depth = south_halo[base : base + 1]
    depth_north = jnp.where(last_row, north_halo[base : base + 1], pltpu.roll(depth, rows - 1, 0))
    open_north = jnp.minimum(depth, depth_north)
    open_south = jnp.minimum(depth[0:1], south_depth)
    open_east = jnp.where(last_lane, 0.0, jnp.minimum(depth, pltpu.roll(depth, LANES - 1, 1)))
    per_area = time_step / area[...]
    edge_level = (lane_of((8, LANES)) // blocks).astype(jnp.float32)
    west_edge, east_edge = [], []
    for f in range(2):
        own_west, own_east = west_own[8 * f : 8 * f + 8], east_own[8 * f : 8 * f + 8]
        west_edge.append(
            edge_flux(west_halo[8 * f : 8 * f + 8], own_west, west_halo[24:32], west_halo[16:24], west_own[16:24], edge_level)
        )
        east_edge.append(
            edge_flux(own_east, east_halo[8 * f : 8 * f + 8], east_own[24:32], east_own[16:24], east_halo[16:24], edge_level)
        )
    fields = (heat, salt)

    def one_level(k, above):
        level = k.astype(jnp.float32)
        east_speed, north_speed = currents[0, k], currents[1, k]
        south_speed = south_halo[pl.ds(base + 8 + k, 1)]
        east_up, east_down = jnp.maximum(east_speed, 0.0), jnp.minimum(east_speed, 0.0)
        north_up, north_down = jnp.maximum(north_speed, 0.0), jnp.minimum(north_speed, 0.0)
        east_wet = level < open_east
        north_wet = level < open_north
        wet = level < depth
        below_wet = level + 1.0 < depth
        passed = []
        for f in range(2):
            cells = fields[f][k]
            at = f * levels + k
            east_flux = jnp.where(
                east_wet, open_flux(cells, pltpu.roll(cells, LANES - 1, 1), east_up, east_down), 0.0
            )
            west_flux = pltpu.roll(east_flux, 1, 1)
            west_columns, east_columns = [], []
            for block in range(blocks):
                place = k * blocks + block
                west_columns.append(pltpu.roll(west_edge[f], (LANES - place) % LANES, 1))
                east_columns.append(pltpu.roll(east_edge[f], LANES - 1 - place, 1))
            west_flux = jnp.where(first_lane, jnp.concatenate(west_columns, axis=0), west_flux)
            east_flux = jnp.where(last_lane, jnp.concatenate(east_columns, axis=0), east_flux)
            northern = jnp.where(last_row, north_halo[pl.ds(at, 1)], pltpu.roll(cells, rows - 1, 0))
            north_flux = jnp.where(north_wet, open_flux(cells, northern, north_up, north_down), 0.0)
            first_flux = edge_flux(
                south_halo[pl.ds(at, 1)], cells[0:1], south_speed, open_south, open_south, level
            )
            south_flux = jnp.where(first_row, first_flux, pltpu.roll(north_flux, 1, 0))
            next_cells = fields[f][jnp.minimum(k + 1, levels - 1)]
            below = jnp.where(below_wet, vertical_mixing * (cells - next_cells), 0.0)
            change = per_area * (west_flux - east_flux + south_flux - north_flux) + time_step * (above[f] - below)
            (heat_out, salt_out)[f][k] = cells + jnp.where(wet, change, 0.0)
            passed.append(below)
        return tuple(passed)

    nothing = jnp.zeros((rows, LANES), jnp.float32)
    lax.fori_loop(0, levels, one_level, (nothing, nothing))


def tracer_step(*arrays):
    heat = arrays[0]
    return pl.pallas_call(
        step_kernel,
        in_specs=[VMEM] * 12,
        out_specs=[VMEM] * 2,
        out_shape=[jax.ShapeDtypeStruct(heat.shape, jnp.float32)] * 2,
        name="tracer_step",
    )(*arrays)


def fold_kernel(heat_next, salt_next, own, fold, area, heat_out, salt_out):
    levels, band, _ = heat_next.shape
    base = 2 * levels
    level = lax.broadcasted_iota(jnp.int32, (levels, LANES), 0).astype(jnp.float32)
    per_area = time_step / area[band - 1 : band]
    speed = 0.5 * (own[base + 8 :] - fold[base:])
    last = lax.broadcasted_iota(jnp.int32, (band, LANES), 0) == band - 1
    wet = jnp.logical_and(level < own[base : base + 1], fold[levels:base] > 0.0)
    forward, backward = jnp.maximum(speed, 0.0), jnp.minimum(speed, 0.0)
    for f, (before, after) in enumerate(((heat_next, heat_out), (salt_next, salt_out))):
        near, far = own[f * levels : f * levels + levels], fold[f * levels : f * levels + levels]
        flux = jnp.where(wet, open_flux(near, far, forward, backward), 0.0)
        leaving = per_area * flux
        for k in range(levels):
            after[k] = before[k] - jnp.where(last, leaving[k : k + 1], 0.0)


def close_fold(heat_next, salt_next, own, fold, area):
    levels, height, width = heat_next.shape
    band = pl.BlockSpec((levels, 8, width), lambda i: (0, height // 8 - 1, 0))
    own_rows, fold_rows = (pl.BlockSpec(rows.shape, lambda i: (0, 0)) for rows in (own, fold))
    return pl.pallas_call(
        fold_kernel,
        grid=(1,),
        in_specs=[band, band, own_rows, fold_rows, pl.BlockSpec((8, width), lambda i: (height // 8 - 1, 0))],
        out_specs=[band, band],
        out_shape=[jax.ShapeDtypeStruct(heat_next.shape, jnp.float32)] * 2,
        input_output_aliases={0: 0, 1: 1},
        name="close_fold",
    )(heat_next, salt_next, own, fold, area)


def final_kernel(salt_next, surface, rain, sea, totals, out):
    lane = lane_of((1, LANES))

    def total(place):
        return jnp.sum(jnp.where(lane == place, totals[...], 0.0), axis=1, keepdims=True)

    total_area, total_fresh, salt_fresh, salt_only = (total(place) for place in range(4))
    mean_fresh = total_fresh / total_area
    total_salt = salt_fresh - mean_fresh * salt_only
    balanced = rain[...] - mean_fresh
    virtual = -surface[0] * balanced + total_salt / total_area
    wet = (sea[...] > 0).astype(jnp.float32)
    out[0] = salt_next[0] + time_step / top_thickness * virtual * wet


def add_virtual(salt_next, brine, rain, sea, totals):
    _, rows, width = salt_next.shape
    plane = pl.BlockSpec((rows, width), lambda i: (0, 0))
    top = pl.BlockSpec((1, rows, width), lambda i: (0, 0, 0))
    return pl.pallas_call(
        final_kernel,
        grid=(1,),
        in_specs=[top, top, plane, plane, pl.BlockSpec((1, LANES), lambda i: (0, 0))],
        out_specs=top,
        out_shape=jax.ShapeDtypeStruct(salt_next.shape, jnp.float32),
        input_output_aliases={0: 0},
        name="add_virtual",
    )(salt_next, brine, rain, sea, totals)


def share(copies, axes):
    return lax.all_to_all(copies, axes, 0, 0, tiled=True)


def along(block, axis, by, closed):
    count = lax.axis_size(axis)
    pairs = [(i, (i + by) % count) for i in range(count) if closed or i + by in range(count)]
    return lax.ppermute(block, axis, pairs)


def fold_branches(beside):
    around, height = lax.axis_size(GX), lax.axis_size("gy")

    def mirror(coarse):
        pairs = [
            (i * height + height - 1, (3 * coarse - i) % around * height + height - 1) for i in range(around)
        ]

        def branch(rows, arrays):
            return lax.ppermute(rows, GX + ("gy",), pairs), beside(*arrays)

        return branch

    return [mirror(coarse) for coarse in range((around + 2) // 3)]


def shards(heat, brine, currents, sea, layers, area, rain, seam):
    _, _, width = heat.shape
    sums = local_sums(brine, sea, area, rain, lax.axis_size(NEAR))
    plane = jnp.sum(share(sums, NEAR), axis=0)
    centre = (seam[0] // width + lax.axis_index(GX)) % lax.axis_size(GX)
    place, part = (centre + 1) // 3, (centre + 1) % 3
    layers, place, part = lax.optimization_barrier((layers, place, part))
    west_own, east_own, south_own, north_own, fold_own = packs(heat, brine, currents, sea, layers)
    totals = share(jnp.broadcast_to(plane[None], (lax.axis_size("chip"),) + plane.shape), "chip")
    totals = jnp.sum(totals, axis=0)
    west_halo = along(east_own, GX, 1, True)
    east_halo = along(west_own, GX, -1, True)
    north_halo = along(south_own, "gy", -1, False)
    south_halo = along(north_own, "gy", 1, False)
    held = jnp.where(part == 0, west_halo[32:], jnp.where(part == 2, east_halo[24:], fold_own))
    arrays = (
        heat, brine, currents, sea, layers, area,
        west_own, east_own, west_halo, east_halo, south_halo, north_halo,
    )
    fold_halo, (heat_next, salt_next) = lax.switch(place, fold_branches(tracer_step), held, arrays)
    heat_next, salt_next = close_fold(heat_next, salt_next, north_own, fold_halo, area)
    return heat_next, add_virtual(salt_next, brine, rain, sea, totals)


def solution(mesh):
    chips = mesh.shape["gx"] // CORES
    split = Mesh(
        mesh.devices.reshape(mesh.shape["groups"], chips, CORES, mesh.shape["gy"]), ("groups",) + GX + ("gy",)
    )
    cells = P("groups", "gy", GX)
    plane = P("gy", GX)
    in_specs = (cells, cells, P("groups", None, "gy", GX), plane, plane, plane, plane, P(GX))
    return jax.shard_map(
        shards, mesh=split, in_specs=in_specs, out_specs=(cells, cells), check_vma=False
    )
```

```python
import jax
import jax.numpy as jnp
from jax import lax
from jax.experimental import pallas as pl
from jax.experimental.pallas import tpu as pltpu
from jax.sharding import Mesh
from jax.sharding import PartitionSpec as P


time_step = 0.25
diffusivity = 0.5
vertical_mixing = 0.3
top_thickness = 0.5

VMEM = pl.BlockSpec(memory_space=pltpu.VMEM)
LANES = 128
CORES = 2
GX = ("chip", "core")
NEAR = ("core", "gy")


def lane_of(shape):
    return lax.broadcasted_iota(jnp.int32, shape, len(shape) - 1)


def sums_kernel(surface, sea, area, rain, out):
    wet_area = area[...] * sea[...].astype(jnp.float32)
    salt = wet_area * surface[0]
    rain_now = rain[...]
    lane = lane_of((1, LANES))
    packed = jnp.zeros((1, LANES), jnp.float32)
    for place, field in enumerate((wet_area, wet_area * rain_now, salt * rain_now, salt)):
        total = jnp.sum(jnp.sum(field, axis=0, keepdims=True), axis=1, keepdims=True)
        packed = jnp.where(lane == place, total, packed)
    out[...] = jnp.broadcast_to(packed[None], out.shape)


def local_sums(brine, sea, area, rain, copies):
    rows, width = sea.shape
    plane = pl.BlockSpec((rows, width), lambda i: (0, 0))
    return pl.pallas_call(
        sums_kernel,
        grid=(1,),
        in_specs=[pl.BlockSpec((1, rows, width), lambda i: (0, 0, 0)), plane, plane, plane],
        out_specs=pl.BlockSpec((copies, 1, LANES), lambda i: (0, 0, 0)),
        out_shape=jax.ShapeDtypeStruct((copies, 1, LANES), jnp.float32),
        name="local_sums",
    )(brine, sea, area, rain)


def mirrored(rows):
    lane = lane_of(rows.shape)
    bit = 1
    while bit < LANES:
        low = (lane // bit) % 2 == 0
        rows = jnp.where(low, pltpu.roll(rows, LANES - bit, 1), pltpu.roll(rows, bit, 1))
        bit *= 2
    return rows


def column_pack(planes, lane_number):
    lane = lane_of((8, LANES))
    blocks = planes[0].shape[0] // 8
    packed = jnp.zeros((8, LANES), jnp.float32)
    for level, plane in enumerate(planes):
        for block in range(blocks):
            place = level * blocks + block
            tile = plane[8 * block : 8 * block + 8]
            moved = pltpu.roll(tile, (place - lane_number) % LANES, 1)
            packed = jnp.where(lane == place, moved, packed)
    return packed


def pack_kernel(heat, salt, currents, sea, layers, west, east, south, north, fold):
    levels, rows, _ = heat.shape
    depth = (sea[...] * layers[...]).astype(jnp.float32)
    heat_planes = [heat[k] for k in range(levels)]
    salt_planes = [salt[k] for k in range(levels)]
    speed_planes = [currents[0, k] for k in range(levels)]
    depth_planes = [depth] * levels
    west[0:8] = column_pack(heat_planes, 0)
    west[8:16] = column_pack(salt_planes, 0)
    west[16:24] = column_pack(depth_planes, 0)
    east[0:8] = column_pack(heat_planes, LANES - 1)
    east[8:16] = column_pack(salt_planes, LANES - 1)
    east[16:24] = column_pack(depth_planes, LANES - 1)
    east[24:32] = column_pack(speed_planes, LANES - 1)
    last = rows - 1
    for k in range(levels):
        south[k : k + 1] = heat[k, 0:1]
        south[levels + k : levels + k + 1] = salt[k, 0:1]
        north[k : k + 1] = heat[k, last:rows]
        north[levels + k : levels + k + 1] = salt[k, last:rows]
        north[2 * levels + 8 + k : 2 * levels + 9 + k] = currents[1, k, last:rows]
    south[2 * levels : 2 * levels + 8] = jnp.broadcast_to(depth[0:1], (8, LANES))
    north[2 * levels : 2 * levels + 8] = jnp.broadcast_to(depth[last:rows], (8, LANES))
    level = lax.broadcasted_iota(jnp.int32, (levels, LANES), 0).astype(jnp.float32)
    fold[0:levels] = mirrored(north[0:levels])
    fold[levels : 2 * levels] = mirrored(
        jnp.where(level < depth[last:rows], north[levels : 2 * levels], 0.0)
    )
    fold[2 * levels :] = mirrored(north[2 * levels + 8 :])
    west[24:] = fold[...]
    east[32:] = fold[...]


def packs(heat, salt, currents, sea, layers):
    levels, _, _ = heat.shape
    north = 3 * levels + 8
    shapes = (24 + 3 * levels, 32 + 3 * levels, 2 * levels + 8, north, 3 * levels)
    return pl.pallas_call(
        pack_kernel,
        in_specs=[VMEM] * 5,
        out_specs=[VMEM] * 5,
        out_shape=[jax.ShapeDtypeStruct((n, LANES), jnp.float32) for n in shapes],
        name="edge_packs",
    )(heat, salt, currents, sea, layers)


def open_flux(near, far, forward, backward):
    return forward * near + backward * far - diffusivity * (far - near)


def edge_flux(near, far, speed, near_depth, far_depth, level):
    wet = (level < jnp.minimum(near_depth, far_depth)).astype(jnp.float32)
    return wet * open_flux(near, far, jnp.maximum(speed, 0.0), jnp.minimum(speed, 0.0))


def step_kernel(
    heat, salt, currents, sea, layers, area,
    west_own, east_own, west_halo, east_halo, north_halo,
    heat_out, salt_out,
):
    levels, rows, _ = heat.shape
    blocks = rows // 8
    lane = lane_of((rows, LANES))
    row = lax.broadcasted_iota(jnp.int32, (rows, LANES), 0)
    first_lane, last_lane = lane == 0, lane == LANES - 1
    first_row, last_row = row == 0, row == rows - 1
    depth = (sea[...] * layers[...]).astype(jnp.float32)
    base = 2 * levels
    depth_north = jnp.where(last_row, north_halo[base : base + 1], pltpu.roll(depth, rows - 1, 0))
    open_north = jnp.minimum(depth, depth_north)
    open_east = jnp.where(last_lane, 0.0, jnp.minimum(depth, pltpu.roll(depth, LANES - 1, 1)))
    per_area = time_step / area[...]
    edge_level = (lane_of((8, LANES)) // blocks).astype(jnp.float32)
    west_edge, east_edge = [], []
    for f in range(2):
        own_west, own_east = west_own[8 * f : 8 * f + 8], east_own[8 * f : 8 * f + 8]
        west_edge.append(
            edge_flux(west_halo[8 * f : 8 * f + 8], own_west, west_halo[24:32], west_halo[16:24], west_own[16:24], edge_level)
        )
        east_edge.append(
            edge_flux(own_east, east_halo[8 * f : 8 * f + 8], east_own[24:32], east_own[16:24], east_halo[16:24], edge_level)
        )
    fields = (heat, salt)

    def one_level(k, above):
        level = k.astype(jnp.float32)
        east_speed, north_speed = currents[0, k], currents[1, k]
        east_up, east_down = jnp.maximum(east_speed, 0.0), jnp.minimum(east_speed, 0.0)
        north_up, north_down = jnp.maximum(north_speed, 0.0), jnp.minimum(north_speed, 0.0)
        east_wet = level < open_east
        north_wet = level < open_north
        wet = level < depth
        below_wet = level + 1.0 < depth
        passed = []
        for f in range(2):
            cells = fields[f][k]
            at = f * levels + k
            east_flux = jnp.where(
                east_wet, open_flux(cells, pltpu.roll(cells, LANES - 1, 1), east_up, east_down), 0.0
            )
            west_flux = pltpu.roll(east_flux, 1, 1)
            west_columns, east_columns = [], []
            for block in range(blocks):
                place = k * blocks + block
                west_columns.append(pltpu.roll(west_edge[f], (LANES - place) % LANES, 1))
                east_columns.append(pltpu.roll(east_edge[f], LANES - 1 - place, 1))
            west_flux = jnp.where(first_lane, jnp.concatenate(west_columns, axis=0), west_flux)
            east_flux = jnp.where(last_lane, jnp.concatenate(east_columns, axis=0), east_flux)
            northern = jnp.where(last_row, north_halo[pl.ds(at, 1)], pltpu.roll(cells, rows - 1, 0))
            north_flux = jnp.where(north_wet, open_flux(cells, northern, north_up, north_down), 0.0)
            south_flux = jnp.where(first_row, 0.0, pltpu.roll(north_flux, 1, 0))
            next_cells = fields[f][jnp.minimum(k + 1, levels - 1)]
            below = jnp.where(below_wet, vertical_mixing * (cells - next_cells), 0.0)
            change = per_area * (west_flux - east_flux + south_flux - north_flux) + time_step * (above[f] - below)
            (heat_out, salt_out)[f][k] = cells + jnp.where(wet, change, 0.0)
            passed.append(below)
        return tuple(passed)

    nothing = jnp.zeros((rows, LANES), jnp.float32)
    lax.fori_loop(0, levels, one_level, (nothing, nothing))


def tracer_step(*arrays):
    heat = arrays[0]
    return pl.pallas_call(
        step_kernel,
        in_specs=[VMEM] * 11,
        out_specs=[VMEM] * 2,
        out_shape=[jax.ShapeDtypeStruct(heat.shape, jnp.float32)] * 2,
        name="tracer_step",
    )(*arrays)


def close_kernel(heat_next, salt_next, south_own, north_own, south_halo, fold, area, heat_out, salt_out):
    levels, band, _ = heat_next.shape
    base = 2 * levels
    level = lax.broadcasted_iota(jnp.int32, (levels, LANES), 0).astype(jnp.float32)
    row = lax.broadcasted_iota(jnp.int32, (band, LANES), 0)
    fields = ((heat_next, heat_out), (salt_next, salt_out))

    def cells(rows, f):
        return rows[f * levels : f * levels + levels]

    @pl.when(pl.program_id(0) == 0)
    def _():
        for f, (before, after) in enumerate(fields):
            flux = edge_flux(
                cells(south_halo, f), cells(south_own, f), south_halo[base + 8 :],
                south_halo[base : base + 1], south_own[base : base + 1], level,
            )
            entering = time_step / area[0:1] * flux
            for k in range(levels):
                after[k] = before[k] + jnp.where(row == 0, entering[k : k + 1], 0.0)

    @pl.when(pl.program_id(0) == 1)
    def _():
        speed = 0.5 * (north_own[base + 8 :] - fold[base:])
        wet = jnp.logical_and(level < north_own[base : base + 1], fold[levels:base] > 0.0)
        forward, backward = jnp.maximum(speed, 0.0), jnp.minimum(speed, 0.0)
        for f, (before, after) in enumerate(fields):
            flux = jnp.where(wet, open_flux(cells(north_own, f), cells(fold, f), forward, backward), 0.0)
            leaving = time_step / area[band - 1 : band] * flux
            for k in range(levels):
                after[k] = before[k] - jnp.where(row == band - 1, leaving[k : k + 1], 0.0)


def close_edges(heat_next, salt_next, south_own, north_own, south_halo, fold, area):
    levels, height, width = heat_next.shape
    gap = height // 8 - 1
    band = pl.BlockSpec((levels, 8, width), lambda i: (0, i * gap, 0))
    packs = (south_own, north_own, south_halo, fold)
    return pl.pallas_call(
        close_kernel,
        grid=(2,),
        in_specs=[band, band]
        + [pl.BlockSpec(rows.shape, lambda i: (0, 0)) for rows in packs]
        + [pl.BlockSpec((8, width), lambda i: (i * gap, 0))],
        out_specs=[band, band],
        out_shape=[jax.ShapeDtypeStruct(heat_next.shape, jnp.float32)] * 2,
        input_output_aliases={0: 0, 1: 1},
        name="close_edges",
    )(heat_next, salt_next, *packs, area)


def final_kernel(salt_next, surface, rain, sea, totals, out):
    lane = lane_of((1, LANES))

    def total(place):
        return jnp.sum(jnp.where(lane == place, totals[...], 0.0), axis=1, keepdims=True)

    total_area, total_fresh, salt_fresh, salt_only = (total(place) for place in range(4))
    mean_fresh = total_fresh / total_area
    total_salt = salt_fresh - mean_fresh * salt_only
    balanced = rain[...] - mean_fresh
    virtual = -surface[0] * balanced + total_salt / total_area
    wet = (sea[...] > 0).astype(jnp.float32)
    out[0] = salt_next[0] + time_step / top_thickness * virtual * wet


def add_virtual(salt_next, brine, rain, sea, totals):
    _, rows, width = salt_next.shape
    plane = pl.BlockSpec((rows, width), lambda i: (0, 0))
    top = pl.BlockSpec((1, rows, width), lambda i: (0, 0, 0))
    return pl.pallas_call(
        final_kernel,
        grid=(1,),
        in_specs=[top, top, plane, plane, pl.BlockSpec((1, LANES), lambda i: (0, 0))],
        out_specs=top,
        out_shape=jax.ShapeDtypeStruct(salt_next.shape, jnp.float32),
        input_output_aliases={0: 0},
        name="add_virtual",
    )(salt_next, brine, rain, sea, totals)


def share(copies, axes):
    return lax.all_to_all(copies, axes, 0, 0, tiled=True)


def along(block, axis, by, closed):
    count = lax.axis_size(axis)
    pairs = [(i, (i + by) % count) for i in range(count) if closed or i + by in range(count)]
    return lax.ppermute(block, axis, pairs)


def fold_branches(beside):
    around, height = lax.axis_size(GX), lax.axis_size("gy")

    def mirror(coarse):
        pairs = [
            (i * height + height - 1, (3 * coarse - i) % around * height + height - 1) for i in range(around)
        ]

        def branch(rows, arrays, south_own):
            fold_halo = lax.ppermute(rows, GX + ("gy",), pairs)
            north_halo = along(south_own, "gy", -1, False)
            return fold_halo, beside(*arrays, north_halo)

        return branch

    return [mirror(coarse) for coarse in range((around + 2) // 3)]


def shards(heat, brine, currents, sea, layers, area, rain, seam):
    _, _, width = heat.shape
    sums = local_sums(brine, sea, area, rain, lax.axis_size(NEAR))
    plane = jnp.sum(share(sums, NEAR), axis=0)
    centre = (seam[0] // width + lax.axis_index(GX)) % lax.axis_size(GX)
    place, part = (centre + 1) // 3, (centre + 1) % 3
    layers, place, part = lax.optimization_barrier((layers, place, part))
    west_own, east_own, south_own, north_own, fold_own = packs(heat, brine, currents, sea, layers)
    totals = share(jnp.broadcast_to(plane[None], (lax.axis_size("chip"),) + plane.shape), "chip")
    totals = jnp.sum(totals, axis=0)
    west_halo = along(east_own, GX, 1, True)
    east_halo = along(west_own, GX, -1, True)
    south_halo = along(north_own, "gy", 1, False)
    held = jnp.where(part == 0, west_halo[32:], jnp.where(part == 2, east_halo[24:], fold_own))
    arrays = (heat, brine, currents, sea, layers, area, west_own, east_own, west_halo, east_halo)
    fold_halo, (heat_next, salt_next) = lax.switch(
        place, fold_branches(tracer_step), held, arrays, south_own
    )
    south_halo, fold_halo = lax.optimization_barrier((south_halo, fold_halo))
    heat_next, salt_next = close_edges(
        heat_next, salt_next, south_own, north_own, south_halo, fold_halo, area
    )
    return heat_next, add_virtual(salt_next, brine, rain, sea, totals)


def solution(mesh):
    chips = mesh.shape["gx"] // CORES
    split = Mesh(
        mesh.devices.reshape(mesh.shape["groups"], chips, CORES, mesh.shape["gy"]), ("groups",) + GX + ("gy",)
    )
    cells = P("groups", "gy", GX)
    plane = P("gy", GX)
    in_specs = (cells, cells, P("groups", None, "gy", GX), plane, plane, plane, plane, P(GX))
    return jax.shard_map(
        shards, mesh=split, in_specs=in_specs, out_specs=(cells, cells), check_vma=False
    )
```
